32 devices in a mesh: seg: 4 (over z), cp: 8 (over y, x, core).
Axes of the slice: x: 2, y: 2, z: 4, core: 2. Of those that a mesh axis runs over, the one named last changes fastest.
Arguments:
- mixed_qkv: bfloat16 [4096, 8192], P(('seg', 'cp')), may hold values from -6 to 6
- gate_z: bfloat16 [4096, 4096], P(('seg', 'cp')), may hold values from -6 to 6
- gate_logits: bfloat16 [4096, 64], P(('seg', 'cp')), may hold values from -16 to 4
- block_table: int32 [4, 16], P('seg'), may hold values from 0 to 15, as said below
- conv_weight: float32 [4, 8192], replicated, may hold values from -3 to 3
- a_log: float32 [32], replicated, may hold values from -0.7 to 0.7
- dt_bias: float32 [32], replicated, may hold values from -0.5 to 0.5
- norm_gain: float32 [128], replicated, may hold values from 0.25 to 1.75
Outputs:
- mixed_out: bfloat16 [4096, 4096], P(('seg', 'cp'))
The draws below stay inside these ranges and needn't reach their ends.
Inputs may be any that keep to these rules, and one draw needn't show every extreme that they name: Each row of block_table is a permutation of the numbers 0 to 15; its entries at even positions are below 8, those at odd positions are 8 or more.
All inputs are finite; a program needn't handle non-finite values.
Results may differ from the reference program's by a relative error of at most 0.001.
Values may be sent and summed in bfloat16 or wider, within the bound.
No kernel may reach another device: no remote copies, remote signals or barrier semaphores. Data moves between devices by JAX's collectives and lax.ppermute only.
A program may use at most 128 MiB of HBM per device.

```python
import jax
import jax.numpy as jnp
from jax import lax

VALUE_HEADS = 32
KEY_HEADS = 16
HEAD_DIM = 128
CONV = 4
BLOCK = 128
TOK_DEV = 128
SEQUENCE_TOKENS = 4096
N_SEG = 4
N_CP = 8


def draw_gate_logits(key, part):
    random_subkeys = jax.random.split(key, 9)
    slow_share = 0.5
    beta_noise = 0.5 * jax.random.normal(random_subkeys[4], (SEQUENCE_TOKENS, VALUE_HEADS), jnp.float32)
    slow_heads = jax.random.uniform(random_subkeys[0], (VALUE_HEADS,), jnp.float32) < slow_share
    beta_base = jnp.where(slow_heads, jax.random.uniform(random_subkeys[1], (VALUE_HEADS,), jnp.float32, -7.0, -5.0), jax.random.uniform(random_subkeys[2], (VALUE_HEADS,), jnp.float32, -1.0, 2.0))
    decay_base = jnp.where(slow_heads, jax.random.uniform(random_subkeys[3], (VALUE_HEADS,), jnp.float32, -13.0, -11.0), jax.random.uniform(random_subkeys[5], (VALUE_HEADS,), jnp.float32, -4.0, -3.0))
    rows_per_half = TOK_DEV // 2
    group_count = SEQUENCE_TOKENS // rows_per_half
    offsets = jax.random.uniform(random_subkeys[6], (group_count, 1, VALUE_HEADS), jnp.float32, -0.7, 0.7)
    offsets = jnp.broadcast_to(offsets, (group_count, rows_per_half, VALUE_HEADS)).reshape(SEQUENCE_TOKENS, VALUE_HEADS)
    beta_logit = beta_base + beta_noise
    decay_logit_raw = decay_base + offsets + 0.3 * jax.random.normal(random_subkeys[7], (SEQUENCE_TOKENS, VALUE_HEADS), jnp.float32)
    doubling_rows = jax.random.uniform(random_subkeys[8], (SEQUENCE_TOKENS, 1), jnp.float32) < 6.0 / SEQUENCE_TOKENS
    doubling_level = jax.random.uniform(jax.random.fold_in(random_subkeys[8], 7), (SEQUENCE_TOKENS, VALUE_HEADS), jnp.float32, -1.0, 0.0)
    decay_logit_raw = jnp.where(doubling_rows, jnp.maximum(decay_logit_raw, doubling_level), decay_logit_raw)
    joined = jnp.concatenate([beta_logit, decay_logit_raw], axis=1)
    return jnp.clip(joined, -16.0, 4.0).astype(jnp.bfloat16)


def draw_block_table(key, part):
    base = jax.random.fold_in(key, 41)
    first_keys = jax.random.split(jax.random.fold_in(base, 1), N_SEG)
    second_keys = jax.random.split(jax.random.fold_in(base, 2), N_SEG)
    first = jax.vmap(lambda one: jax.random.permutation(one, N_CP))(first_keys).astype(jnp.int32)
    second = jax.vmap(lambda one: jax.random.permutation(one, N_CP))(second_keys).astype(jnp.int32) + N_CP
    return jnp.stack([first, second], axis=-1).reshape(N_SEG, 2 * N_CP).astype(jnp.int32)


def levels(own_key, shape, cuts, least, largest):
    factor_of = 1.0
    for position, blocks in cuts:
        draws = jax.random.uniform(jax.random.fold_in(jax.random.fold_in(own_key, 6), position), (blocks,), jnp.float32, least / len(cuts), largest / len(cuts))
        factor_of = factor_of * jnp.repeat(jnp.exp(draws), shape[position] // blocks).reshape((-1,) + (1,) * (len(shape) - 1 - position))
    return factor_of


def normal_values(own_key, shape, deviation, most, cuts=(), kind=jnp.bfloat16):
    factor_of = levels(own_key, shape, cuts, -0.22, 0.18) if cuts else 1.0
    values = jax.random.normal(own_key, shape, jnp.float32) * deviation * factor_of
    return jnp.minimum(jnp.maximum(values, -most), most).astype(kind)


def setup_inputs(seed: int = 0) -> dict:
    seeds = jax.random.split(jax.random.key(seed), 9)
    return {
        "mixed_qkv": normal_values(seeds[0], (SEQUENCE_TOKENS, 2 * KEY_HEADS * HEAD_DIM + VALUE_HEADS * HEAD_DIM), 1.0, 6.0, ((0, 32),)),
        "gate_z": normal_values(seeds[1], (SEQUENCE_TOKENS, VALUE_HEADS * HEAD_DIM), 1.0, 6.0, ((0, 32),)),
        "gate_logits": draw_gate_logits(jax.random.fold_in(seeds[8], 71), 0),
        "block_table": draw_block_table(jax.random.fold_in(seeds[8], 71), 0),
        "conv_weight": normal_values(seeds[4], (CONV, 2 * KEY_HEADS * HEAD_DIM + VALUE_HEADS * HEAD_DIM), CONV ** -0.5, 3.0, (), jnp.float32),
        "a_log": jnp.clip(jax.random.uniform(seeds[5], (VALUE_HEADS,), jnp.float32, -0.7, 0.7), -0.7, 0.7),
        "dt_bias": jnp.clip(jax.random.uniform(seeds[6], (VALUE_HEADS,), jnp.float32, -0.5, 0.5), -0.5, 0.5),
        "norm_gain": jnp.clip(1.0 + 0.15 * jax.random.normal(seeds[7], (HEAD_DIM,), jnp.float32), 0.25, 1.75),
    }


highest = lax.Precision.HIGHEST

def to_sequence(stored, table):
    columns = stored.shape[1]
    pieces = stored.reshape(N_SEG, 2 * N_CP, TOK_DEV // 2, columns)
    order = jnp.argsort(table, axis=1).astype(jnp.int32)
    picked = jnp.take_along_axis(pieces, order[:, :, None, None], axis=1)
    return picked.reshape(stored.shape[0], columns)

def causal_conv(rows, weights):
    padded = jnp.pad(rows, ((CONV - 1, 0), (0, 0)))
    length = rows.shape[0]
    summed = jnp.zeros(rows.shape, jnp.float32)
    for offset in range(CONV):
        summed = summed + weights[offset] * padded[offset:offset + length].astype(jnp.float32)
    return jax.nn.silu(summed)

def unit_rows(matrix):
    return matrix * lax.rsqrt(lax.optimization_barrier(jnp.sum(matrix * matrix, axis=-1, keepdims=True)) + 1e-06)

def block_terms(queries, key_rows, values, beta_rate, decays):
    cumulative = jnp.cumsum(decays, axis=-1)
    final_sum = cumulative[..., -1:]
    spread = cumulative[..., :, None] - cumulative[..., None, :]
    row_index = lax.broadcasted_iota(jnp.int32, (BLOCK, BLOCK), 0)
    col_index = lax.broadcasted_iota(jnp.int32, (BLOCK, BLOCK), 1)
    strict = row_index > col_index
    inclusive = row_index >= col_index
    strict_decay = jnp.where(strict, jnp.exp(jnp.where(strict, spread, 0.0)), 0.0)
    incl_decay = jnp.where(inclusive, jnp.exp(jnp.where(inclusive, spread, 0.0)), 0.0)
    weighted = key_rows * beta_rate[..., None]
    lower = jnp.einsum('...cd,...ed->...ce', weighted, key_rows, precision=highest) * strict_decay
    system = lower + jnp.eye(BLOCK, dtype=jnp.float32)
    right_side = jnp.concatenate([values * beta_rate[..., None], weighted * jnp.exp(cumulative)[..., None]], axis=-1)
    solved = jax.scipy.linalg.solve_triangular(system, right_side, lower=True, unit_diagonal=True)
    corrected = solved[..., :HEAD_DIM]
    projector = solved[..., HEAD_DIM:]
    key_decay = key_rows * jnp.exp(final_sum - cumulative)[..., None]
    query_decay = queries * jnp.exp(cumulative)[..., None]
    scores = jnp.einsum('...cd,...ed->...ce', queries, key_rows, precision=highest) * incl_decay
    return (corrected, projector, key_decay, query_decay, scores, jnp.exp(final_sum[..., 0]))

def reference(mixed_qkv, gate_z, gate_logits, block_table, conv_weight, a_log, dt_bias, norm_gain):
    seq_qkv = to_sequence(mixed_qkv, block_table)
    seq_z = to_sequence(gate_z, block_table)
    seq_gates = to_sequence(gate_logits, block_table)
    conv_out = causal_conv(seq_qkv, conv_weight)
    length = conv_out.shape[0]
    key_width = KEY_HEADS * HEAD_DIM
    group_size = VALUE_HEADS // KEY_HEADS
    queries = unit_rows(conv_out[:, :key_width].reshape(length, KEY_HEADS, HEAD_DIM)) * HEAD_DIM ** (-0.5)
    key_rows = unit_rows(conv_out[:, key_width:2 * key_width].reshape(length, KEY_HEADS, HEAD_DIM))
    queries = jnp.repeat(queries, group_size, axis=1)
    key_rows = jnp.repeat(key_rows, group_size, axis=1)
    values = conv_out[:, 2 * key_width:].reshape(length, VALUE_HEADS, HEAD_DIM)
    gate_float = seq_gates.astype(jnp.float32)
    beta_rate = jax.nn.sigmoid(gate_float[:, :VALUE_HEADS])
    decays = -jnp.exp(a_log) * jax.nn.softplus(gate_float[:, VALUE_HEADS:] + dt_bias)
    count = length // BLOCK

    def to_blocks(array):
        return array.reshape(count, BLOCK, VALUE_HEADS, HEAD_DIM).transpose(0, 2, 1, 3)

    def to_block_rates(array):
        return array.reshape(count, BLOCK, VALUE_HEADS).transpose(0, 2, 1)

    def block_step(state, pieces):
        query_block, key_block, value_block, beta_block, decay_block = pieces
        corrected, projector, key_decay, query_decay, scores, last_decay = block_terms(query_block, key_block, value_block, beta_block, decay_block)
        new_values = corrected - jnp.einsum('hcd,hde->hce', projector, state, precision=highest)
        outputs = jnp.einsum('hcd,hde->hce', query_decay, state, precision=highest)
        outputs = outputs + jnp.einsum('hce,hev->hcv', scores, new_values, precision=highest)
        state = last_decay[:, None, None] * state + jnp.einsum('hcd,hce->hde', key_decay, new_values, precision=highest)
        return (state, outputs)
    initial = jnp.zeros((VALUE_HEADS, HEAD_DIM, HEAD_DIM), jnp.float32)
    _, blocked = lax.scan(block_step, initial, (to_blocks(queries), to_blocks(key_rows), to_blocks(values), to_block_rates(beta_rate), to_block_rates(decays)))
    core = blocked.transpose(0, 2, 1, 3).reshape(length, VALUE_HEADS, HEAD_DIM)
    gate_values = seq_z.astype(jnp.float32).reshape(length, VALUE_HEADS, HEAD_DIM)
    scale = lax.rsqrt(lax.optimization_barrier(jnp.mean(core * core, axis=-1, keepdims=True)) + 1e-06)
    normed = core * scale * norm_gain * jax.nn.silu(gate_values)
    return normed.reshape(length, VALUE_HEADS * HEAD_DIM).astype(jnp.bfloat16)
```

```python
import functools

import jax
import jax.numpy as jnp
from jax import lax
from jax.experimental import pallas as pl
from jax.experimental.pallas import tpu as pltpu
from jax.sharding import PartitionSpec as P

VALUE_HEADS = 32
KEY_HEADS = 16
HEAD_DIM = 128
CONV = 4
BLOCK = 128
GROUP = VALUE_HEADS // KEY_HEADS
LEVELS = (2, 4, 8, 16, 32, 64)

F32 = jnp.float32
BF16 = jnp.bfloat16
highest = lax.Precision.HIGHEST


def dot(a, b):
    return jnp.dot(a, b, preferred_element_type=F32)


def split(x):
    high = x.astype(BF16)
    low = (x - high.astype(F32)).astype(BF16)
    return high, low


def beside(*parts):
    return jnp.concatenate(parts, axis=1)


def below(*parts):
    return jnp.concatenate(parts, axis=0)


def narrow_product(a, b):
    row = beside(b[0], b[1])
    both = dot(beside(a[0], a[1]), below(row, row))
    half = row.shape[1] // 2
    return both[:, :half] + both[:, half:]


def wide_product(a, b):
    return dot(beside(a[0], a[1]), below(b[0], b[0])) + dot(a[0], b[1])


def silu(v):
    return v / (1.0 + jnp.exp(-v))


def softplus(v):
    e = jnp.exp(-jnp.abs(v))
    s = e / (2.0 + e)
    t = s * s
    series = 1.0 / 19.0
    for odd in (17, 15, 13, 11, 9, 7, 5, 3, 1):
        series = series * t + 1.0 / odd
    return jnp.maximum(v, 0.0) + 2.0 * s * series


def local_kernel(
    dims,
    order_ref,
    recv_ref,
    tail_ref,
    weight_ref,
    rate_ref,
    out_ref,
    reach_ref,
    final_ref,
    rows_ref,
    mask_ref,
    state_ref,
):
    key_heads, heads, count, per_step = dims
    tiles = 2 * key_heads + heads
    share = heads // key_heads
    piece_rows = BLOCK // 2
    gate_row = tiles * BLOCK

    row_index = lax.broadcasted_iota(jnp.int32, (BLOCK, BLOCK), 0)
    col_index = lax.broadcasted_iota(jnp.int32, (BLOCK, BLOCK), 1)
    differ = row_index ^ col_index
    for place, size in enumerate(LEVELS):
        inside = (differ >= size) & (differ < 2 * size)
        mask_ref[place] = jnp.where(inside, 1.0, 0.0).astype(BF16)
    eye = jnp.where(row_index == col_index, 1.0, 0.0).astype(F32)
    for h in range(heads):
        state_ref[h] = beside(jnp.zeros((HEAD_DIM, HEAD_DIM), F32), eye)

    def step(index, carry):
        blocks = [index * per_step + b for b in range(per_step)]
        keys, queries, values = {}, {}, {}
        for b, n in enumerate(blocks):
            for tile in range(tiles):
                slot = b * tiles + tile
                before = jnp.maximum(2 * n - 1, 0)
                place = order_ref[before]
                start = tile * BLOCK + (place % 2) * piece_rows + piece_rows - 16
                start = pl.multiple_of(start, 16)
                old = recv_ref[place // 2, pl.ds(start, 16), :]
                old = jnp.where(n == 0, tail_ref[tile].astype(F32), old.astype(F32))
                rows_ref[slot, 0:8, :] = old[8:16]
                for half in range(2):
                    place = order_ref[2 * n + half]
                    start = tile * BLOCK + (place % 2) * piece_rows
                    start = pl.multiple_of(start, piece_rows)
                    fresh = recv_ref[place // 2, pl.ds(start, piece_rows), :]
                    rows_ref[slot, 8 + half * piece_rows : 8 + (half + 1) * piece_rows, :] = (
                        fresh.astype(F32)
                    )
                summed = None
                for offset in range(CONV):
                    tap = weight_ref[tile, offset : offset + 1, :]
                    shifted = rows_ref[slot, 8 - CONV + 1 + offset : 8 - CONV + 1 + offset + BLOCK, :]
                    term = tap * shifted
                    summed = term if summed is None else summed + term
                active = silu(summed)
                if tile < 2 * key_heads:
                    norm = lax.rsqrt(jnp.sum(active * active, axis=-1, keepdims=True) + 1e-06)
                    if tile < key_heads:
                        queries[b, tile] = active * (norm * HEAD_DIM ** (-0.5))
                    else:
                        keys[b, tile - key_heads] = active * norm
                else:
                    values[b, tile - 2 * key_heads] = active

        lane = lax.broadcasted_iota(jnp.int32, (16, BLOCK), 1)
        upper = jnp.where(row_index <= col_index, 1.0, 0.0).astype(BF16)
        cum_rows, beta_rows, end_rows, cum_cols = {}, {}, {}, {}
        for b, n in enumerate(blocks):
            picked = []
            for half in range(2):
                place = order_ref[2 * n + half]
                start = pl.multiple_of(gate_row + (place % 2) * 16, 16)
                picked.append(recv_ref[place // 2, pl.ds(start, 16), :].astype(F32))
            logits = jnp.where(lane < piece_rows, picked[0], picked[1])
            beta_rows[b] = 1.0 / (1.0 + jnp.exp(-logits[0:8]))
            decay = -jnp.exp(rate_ref[0]) * softplus(logits[8:16] + rate_ref[1])
            high, rest = split(decay)
            middle_full = decay - high.astype(F32)
            middle = middle_full.astype(BF16)
            low = (middle_full - middle.astype(F32)).astype(BF16)
            stacked = below(high.astype(F32), middle.astype(F32), low.astype(F32))
            stacked = below(stacked, jnp.zeros((8, BLOCK), F32)).astype(BF16)
            sums = dot(stacked, upper)
            cum = sums[0:8] + sums[8:16] + sums[16:24]
            cum_rows[b] = cum
            end_rows[b] = jnp.broadcast_to(cum[:, BLOCK - 1 :], (8, BLOCK))
            padded = below(cum, jnp.zeros((BLOCK - 8, BLOCK), F32))
            cum_cols[b] = padded.T

        strict = row_index > col_index
        inclusive = row_index >= col_index
        flipped, grams = {}, {}
        for b in range(per_step):
            for g in range(key_heads):
                turned = keys[b, g].T
                flipped[b, g] = turned
                k_high, k_low = split(keys[b, g])
                q_high, q_low = split(queries[b, g])
                t_high, t_low = split(turned)
                row = beside(t_high, t_low)
                left = below(beside(k_high, k_low), beside(q_high, q_low))
                both = dot(left, below(row, row))
                gram = both[:, :BLOCK] + both[:, BLOCK:]
                grams[b, g] = (gram[:BLOCK], gram[BLOCK:])

        units = [(b, h) for b in range(per_step) for h in range(heads)]
        system, inverse, attend, grow = {}, {}, {}, {}
        for b, h in units:
            g = h // share
            column = jnp.broadcast_to(cum_cols[b][:, h : h + 1], (BLOCK, BLOCK))
            line = cum_rows[b][h : h + 1]
            decay = jnp.exp(jnp.where(inclusive, column - line, 0.0))
            grow[b, h] = jnp.exp(column)
            scaled = decay * beta_rows[b][h : h + 1]
            gram_key, gram_query = grams[b, g]
            attend[b, h] = split(jnp.where(inclusive, gram_query * scaled, 0.0))
            lower = jnp.where(strict, gram_key * scaled, 0.0)
            system[b, h] = split(lower)
            inverse[b, h] = eye - jnp.where(differ == 1, lower, 0.0)

        for place, size in enumerate(LEVELS):
            mask = mask_ref[place]
            halves, cross = {}, {}
            for u in units:
                halves[u] = split(inverse[u])
                parts = (system[u][0] * mask, system[u][1] * mask)
                cross[u] = split(narrow_product(parts, halves[u]))
            for u in units:
                inverse[u] = inverse[u] - narrow_product(halves[u], cross[u])

        solved = {}
        for b, h in units:
            g = h // share
            right = split(beside(values[b, h], keys[b, g] * grow[b, h]))
            solved[b, h] = wide_product(split(inverse[b, h]), right)

        for b, n in enumerate(blocks):
            for h in range(heads):
                g = h // share
                ux = solved[b, h][:, :HEAD_DIM]
                px = split(solved[b, h][:, HEAD_DIM:])
                state = state_ref[h]
                state_parts = split(state)
                fresh = beside(ux, jnp.zeros((BLOCK, HEAD_DIM), F32)) - wide_product(px, state_parts)
                fresh_parts = split(fresh)
                end = end_rows[b][h : h + 1]
                line = cum_rows[b][h : h + 1]
                weight = jnp.exp(end - line) * beta_rows[b][h : h + 1]
                key_parts = split(flipped[b, g] * weight)
                keep = jnp.exp(end)
                state_ref[h] = state * beside(keep, keep) + wide_product(key_parts, fresh_parts)
                q_high, q_low = split(queries[b, g] * grow[b, h])
                a_high, a_low = attend[b, h]
                right_high = below(state_parts[0], fresh_parts[0])
                right_low = below(state_parts[1], fresh_parts[1])
                left_high = beside(q_high, a_high)
                left_low = beside(q_low, a_low)
                both = dot(left_high, right_high) + dot(left_low, right_high) + dot(left_high, right_low)
                at = pl.multiple_of(n * BLOCK, BLOCK)
                out_ref[h, pl.ds(at, BLOCK), :] = both[:, :HEAD_DIM]
                r_high, r_low = split(both[:, HEAD_DIM:])
                reach_ref[h, pl.ds(at, BLOCK), :] = beside(r_high, r_low)
        return carry

    lax.fori_loop(0, count // per_step, step, 0)
    for h in range(heads):
        final_ref[h] = state_ref[h]


def finish_kernel(dims, order_ref, core_ref, reach_ref, incoming_ref, gate_ref, gain_ref, out_ref):
    heads, count = dims
    piece_rows = BLOCK // 2

    def step(n, carry):
        at = pl.multiple_of(n * BLOCK, BLOCK)
        for h in range(heads):
            high, low = split(incoming_ref[h])
            row = beside(high, low)
            both = dot(reach_ref[h, pl.ds(at, BLOCK), :], below(row, row))
            core = core_ref[h, pl.ds(at, BLOCK), :] + both[:, :HEAD_DIM] + both[:, HEAD_DIM:]
            scale = lax.rsqrt(jnp.mean(core * core, axis=-1, keepdims=True) + 1e-06)
            gates = []
            for half in range(2):
                place = order_ref[2 * n + half]
                start = pl.multiple_of(h * BLOCK + (place % 2) * piece_rows, piece_rows)
                gates.append(gate_ref[place // 2, pl.ds(start, piece_rows), :].astype(F32))
            gate = below(*gates)
            result = core * scale * gain_ref[...] * silu(gate)
            out_ref[n, h * BLOCK : (h + 1) * BLOCK, :] = result.astype(BF16)
        return carry

    lax.fori_loop(0, count, step, 0)


def passed_along(value, axis, by):
    length = lax.axis_size(axis)
    pairs = [(i, i + by) for i in range(length) if 0 <= i + by < length]
    return lax.ppermute(value, axis, pairs)


def per_device(mixed_qkv, gate_z, gate_logits, block_table, conv_weight, a_log, dt_bias, norm_gain):
    cp_count = lax.axis_size("cp")
    seg_count = lax.axis_size("seg")
    cp_place = lax.axis_index("cp")
    rows = mixed_qkv.shape[0]
    heads = VALUE_HEADS // cp_count
    key_heads = max(1, heads // GROUP)
    copies = cp_count * key_heads // KEY_HEADS
    tiles = 2 * key_heads + heads
    key_width = KEY_HEADS * HEAD_DIM
    count = cp_count * rows // BLOCK
    per_step = 2 if count % 2 == 0 else 1
    order = jnp.argsort(block_table[0]).astype(jnp.int32)

    def key_tiles(array, lead):
        shaped = array.reshape(lead, KEY_HEADS, HEAD_DIM)
        if copies > 1:
            shaped = jnp.repeat(shaped, copies, axis=1)
        return shaped.reshape(lead, cp_count, key_heads, HEAD_DIM)

    def value_tiles(array, lead):
        return array.reshape(lead, cp_count, heads, HEAD_DIM)

    def by_tiles(array):
        lead = array.shape[0]
        return (
            key_tiles(array[:, :key_width], lead),
            key_tiles(array[:, key_width : 2 * key_width], lead),
            value_tiles(array[:, 2 * key_width :], lead),
        )

    def to_send(shaped):
        return shaped.transpose(1, 2, 0, 3).reshape(cp_count, -1, HEAD_DIM)

    half_rows = rows // 2
    gates = gate_logits.T.reshape(2, cp_count, heads, 2, half_rows).transpose(1, 3, 0, 2, 4)
    gates = jnp.pad(gates, ((0, 0), (0, 0), (0, 0), (0, 8 - heads), (0, 0)))
    gates = jnp.concatenate([gates, gates], axis=-1).reshape(cp_count, 32, 2 * half_rows)
    sent = jnp.concatenate([to_send(part) for part in by_tiles(mixed_qkv)] + [gates], axis=1)
    received = lax.all_to_all(sent, "cp", split_axis=0, concat_axis=0, tiled=True)
    gate_seq = lax.all_to_all(
        to_send(value_tiles(gate_z, rows)), "cp", split_axis=0, concat_axis=0, tiled=True
    )

    last = order[2 * cp_count - 1]
    last_rows = lax.dynamic_index_in_dim(received, last // 2, 0, keepdims=False)
    tail = last_rows[: tiles * BLOCK].reshape(tiles, BLOCK, HEAD_DIM)
    tail = lax.dynamic_slice_in_dim(tail, (last % 2) * half_rows + half_rows - 16, 16, 1)
    tail = passed_along(tail, "seg", 1)

    weights = jnp.concatenate(
        [
            lax.dynamic_index_in_dim(part, cp_place, 1, keepdims=False)
            for part in by_tiles(conv_weight)
        ],
        axis=1,
    ).transpose(1, 0, 2)
    head_log = lax.dynamic_slice_in_dim(a_log, cp_place * heads, heads, 0)
    head_bias = lax.dynamic_slice_in_dim(dt_bias, cp_place * heads, heads, 0)
    rates = jnp.pad(jnp.stack([head_log, head_bias]), ((0, 0), (0, 8 - heads)))
    rates = jnp.broadcast_to(rates[:, :, None], (2, 8, BLOCK))

    vmem = pl.BlockSpec(memory_space=pltpu.VMEM)
    smem = pl.BlockSpec(memory_space=pltpu.SMEM)
    core, reach, final = pl.pallas_call(
        functools.partial(local_kernel, (key_heads, heads, count, per_step)),
        out_shape=(
            jax.ShapeDtypeStruct((heads, count * BLOCK, HEAD_DIM), F32),
            jax.ShapeDtypeStruct((heads, count * BLOCK, 2 * HEAD_DIM), BF16),
            jax.ShapeDtypeStruct((heads, HEAD_DIM, 2 * HEAD_DIM), F32),
        ),
        in_specs=[smem, vmem, vmem, vmem, vmem],
        out_specs=(vmem, vmem, vmem),
        scratch_shapes=[
            pltpu.VMEM((per_step * tiles, 8 + BLOCK, HEAD_DIM), F32),
            pltpu.VMEM((len(LEVELS), BLOCK, BLOCK), BF16),
            pltpu.VMEM((heads, HEAD_DIM, 2 * HEAD_DIM), F32),
        ],
        cost_estimate=pl.CostEstimate(
            flops=int(2e10), bytes_accessed=int(8e6), transcendentals=int(1e6)
        ),
        name="local",
    )(order, received, tail, weights, rates)

    shift = final[:, :, :HEAD_DIM]
    reach_map = final[:, :, HEAD_DIM:]
    incoming = jnp.zeros((heads, HEAD_DIM, HEAD_DIM), F32)
    for rounds in range(seg_count - 1):
        advanced = shift
        if rounds:
            advanced = shift + jnp.einsum("hij,hjk->hik", reach_map, incoming, precision=highest)
        incoming = passed_along(advanced, "seg", 1)

    blocks = pl.pallas_call(
        functools.partial(finish_kernel, (heads, count)),
        out_shape=jax.ShapeDtypeStruct((count, heads * BLOCK, HEAD_DIM), BF16),
        in_specs=[smem, vmem, vmem, vmem, vmem, vmem],
        out_specs=vmem,
        cost_estimate=pl.CostEstimate(
            flops=int(2e9), bytes_accessed=int(6e6), transcendentals=int(1e6)
        ),
        name="finish",
    )(order, core, reach, incoming, gate_seq, norm_gain.reshape(1, HEAD_DIM))
    swapped = lax.all_to_all(blocks, "cp", split_axis=0, concat_axis=0, tiled=True)
    swapped = swapped.reshape(cp_count, heads, rows, HEAD_DIM)
    return swapped.transpose(2, 0, 1, 3).reshape(rows, VALUE_HEADS * HEAD_DIM)


def solution(mesh):
    return jax.shard_map(
        per_device,
        mesh=mesh,
        in_specs=(
            P(("seg", "cp"), None),
            P(("seg", "cp"), None),
            P(("seg", "cp"), None),
            P("seg", None),
            P(),
            P(),
            P(),
            P(),
        ),
        out_specs=P(("seg", "cp"), None),
        check_vma=False,
    )
```

```python
import functools

import jax
import jax.numpy as jnp
from jax import lax
from jax.experimental import pallas as pl
from jax.experimental.pallas import tpu as pltpu
from jax.sharding import PartitionSpec as P

VALUE_HEADS = 32
KEY_HEADS = 16
HEAD_DIM = 128
CONV = 4
BLOCK = 128
GROUP = VALUE_HEADS // KEY_HEADS
LEVELS = (2, 4, 8, 16, 32, 64)

F32 = jnp.float32
BF16 = jnp.bfloat16
highest = lax.Precision.HIGHEST


def dot(a, b):
    return jnp.dot(a, b, preferred_element_type=F32)


def split(x):
    high = x.astype(BF16)
    low = (x - high.astype(F32)).astype(BF16)
    return high, low


def beside(*parts):
    return jnp.concatenate(parts, axis=1)


def below(*parts):
    return jnp.concatenate(parts, axis=0)


def narrow_product(a, b):
    row = beside(b[0], b[1])
    both = dot(beside(a[0], a[1]), below(row, row))
    half = row.shape[1] // 2
    return both[:, :half] + both[:, half:]


def wide_product(a, b):
    return dot(beside(a[0], a[1]), below(b[0], b[0])) + dot(a[0], b[1])


def silu(v):
    return v / (1.0 + jnp.exp(-v))


def softplus(v):
    e = jnp.exp(-jnp.abs(v))
    s = e / (2.0 + e)
    t = s * s
    series = 1.0 / 19.0
    for odd in (17, 15, 13, 11, 9, 7, 5, 3, 1):
        series = series * t + 1.0 / odd
    return jnp.maximum(v, 0.0) + 2.0 * s * series


def local_kernel(
    dims,
    meta_ref,
    recv_ref,
    logit_ref,
    tail_ref,
    weight_ref,
    rate_ref,
    *refs,
):
    group, share, first_block, count, per_step, gate_row, carried = dims
    if carried:
        given_ref, refs = refs[0], refs[1:]
    out_ref, reach_ref, final_ref, rows_ref, mask_ref, state_ref = refs
    tiles = 2 + share
    piece_rows = BLOCK // 2
    is_first = meta_ref[meta_ref.shape[0] - 1]

    row_index = lax.broadcasted_iota(jnp.int32, (BLOCK, BLOCK), 0)
    col_index = lax.broadcasted_iota(jnp.int32, (BLOCK, BLOCK), 1)
    differ = row_index ^ col_index
    for place, size in enumerate(LEVELS):
        inside = (differ >= size) & (differ < 2 * size)
        mask_ref[place] = jnp.where(inside, 1.0, 0.0).astype(BF16)
    eye = jnp.where(row_index == col_index, 1.0, 0.0).astype(F32)
    for h in range(share):
        if carried:
            state_ref[h] = given_ref[h]
        else:
            state_ref[h] = beside(jnp.zeros((HEAD_DIM, HEAD_DIM), F32), eye)

    def step(index, carry):
        spots = [index * per_step + b for b in range(per_step)]
        blocks = [first_block + spot for spot in spots]
        keys, queries, values = {}, {}, {}
        for b, n in enumerate(blocks):
            for tile in range(tiles):
                slot = b * tiles + tile
                before = jnp.maximum(2 * n - 1, 0)
                place = meta_ref[before]
                start = tile * BLOCK + (place % 2) * piece_rows + piece_rows - 16
                start = pl.multiple_of(start, 16)
                old = recv_ref[place // 2, pl.ds(start, 16), :].astype(F32)
                if first_block == 0:
                    lead = tail_ref[tile].astype(F32)
                    lead = jnp.where(is_first == 1, 0.0, lead)
                    old = jnp.where(n == 0, lead, old)
                rows_ref[slot, 0:8, :] = old[8:16]
                for half in range(2):
                    place = meta_ref[2 * n + half]
                    start = tile * BLOCK + (place % 2) * piece_rows
                    start = pl.multiple_of(start, piece_rows)
                    fresh = recv_ref[place // 2, pl.ds(start, piece_rows), :]
                    rows_ref[slot, 8 + half * piece_rows : 8 + (half + 1) * piece_rows, :] = (
                        fresh.astype(F32)
                    )
                summed = None
                for offset in range(CONV):
                    tap = weight_ref[tile, offset : offset + 1, :]
                    begin = 8 - CONV + 1 + offset
                    term = tap * rows_ref[slot, begin : begin + BLOCK, :]
                    summed = term if summed is None else summed + term
                active = silu(summed)
                if tile < 2:
                    norm = lax.rsqrt(jnp.sum(active * active, axis=-1, keepdims=True) + 1e-06)
                    if tile == 0:
                        queries[b] = active * (norm * HEAD_DIM ** (-0.5))
                    else:
                        keys[b] = active * norm
                else:
                    values[b, tile - 2] = active

        lane = lax.broadcasted_iota(jnp.int32, (16, BLOCK), 1)
        upper = jnp.where(row_index <= col_index, 1.0, 0.0).astype(BF16)
        cum_rows, beta_rows, end_rows, cum_cols = {}, {}, {}, {}
        for b, n in enumerate(blocks):
            picked = []
            for half in range(2):
                place = meta_ref[2 * n + half]
                start = pl.multiple_of(gate_row + (place % 2) * 16, 16)
                picked.append(logit_ref[place // 2, pl.ds(start, 16), :].astype(F32))
            logits = jnp.where(lane < piece_rows, picked[0], picked[1])
            beta_rows[b] = 1.0 / (1.0 + jnp.exp(-logits[0:8]))
            decay = -jnp.exp(rate_ref[0]) * softplus(logits[8:16] + rate_ref[1])
            high, rest = split(decay)
            middle_full = decay - high.astype(F32)
            middle = middle_full.astype(BF16)
            low = (middle_full - middle.astype(F32)).astype(BF16)
            stacked = below(high.astype(F32), middle.astype(F32), low.astype(F32))
            stacked = below(stacked, jnp.zeros((8, BLOCK), F32)).astype(BF16)
            sums = dot(stacked, upper)
            cum = sums[0:8] + sums[8:16] + sums[16:24]
            cum_rows[b] = cum
            end_rows[b] = jnp.broadcast_to(cum[:, BLOCK - 1 :], (8, BLOCK))
            padded = below(cum, jnp.zeros((BLOCK - 8, BLOCK), F32))
            cum_cols[b] = padded.T

        strict = row_index > col_index
        inclusive = row_index >= col_index
        flipped, grams = {}, {}
        for b in range(per_step):
            turned = keys[b].T
            flipped[b] = turned
            k_high, k_low = split(keys[b])
            q_high, q_low = split(queries[b])
            t_high, t_low = split(turned)
            row = beside(t_high, t_low)
            left = below(beside(k_high, k_low), beside(q_high, q_low))
            both = dot(left, below(row, row))
            gram = both[:, :BLOCK] + both[:, BLOCK:]
            grams[b] = (gram[:BLOCK], gram[BLOCK:])

        units = [(b, h) for b in range(per_step) for h in range(share)]
        system, inverse, attend, grow = {}, {}, {}, {}
        for b, h in units:
            at = group * share + h
            column = jnp.broadcast_to(cum_cols[b][:, at : at + 1], (BLOCK, BLOCK))
            line = cum_rows[b][at : at + 1]
            decay = jnp.exp(jnp.where(inclusive, column - line, 0.0))
            grow[b, h] = jnp.exp(column)
            scaled = decay * beta_rows[b][at : at + 1]
            gram_key, gram_query = grams[b]
            attend[b, h] = split(jnp.where(inclusive, gram_query * scaled, 0.0))
            lower = jnp.where(strict, gram_key * scaled, 0.0)
            system[b, h] = split(lower)
            inverse[b, h] = eye - jnp.where(differ == 1, lower, 0.0)

        for place, size in enumerate(LEVELS):
            mask = mask_ref[place]
            halves, cross = {}, {}
            for u in units:
                halves[u] = split(inverse[u])
                parts = (system[u][0] * mask, system[u][1] * mask)
                cross[u] = split(narrow_product(parts, halves[u]))
            for u in units:
                inverse[u] = inverse[u] - narrow_product(halves[u], cross[u])

        solved = {}
        for b, h in units:
            right = split(beside(values[b, h], keys[b] * grow[b, h]))
            solved[b, h] = wide_product(split(inverse[b, h]), right)

        for b, spot in enumerate(spots):
            for h in range(share):
                row = group * share + h
                ux = solved[b, h][:, :HEAD_DIM]
                px = split(solved[b, h][:, HEAD_DIM:])
                state = state_ref[h]
                state_parts = split(state)
                fresh = beside(ux, jnp.zeros((BLOCK, HEAD_DIM), F32)) - wide_product(px, state_parts)
                fresh_parts = split(fresh)
                end = end_rows[b][row : row + 1]
                line = cum_rows[b][row : row + 1]
                weight = jnp.exp(end - line) * beta_rows[b][row : row + 1]
                key_parts = split(flipped[b] * weight)
                keep = jnp.exp(end)
                state_ref[h] = state * beside(keep, keep) + wide_product(key_parts, fresh_parts)
                q_high, q_low = split(queries[b] * grow[b, h])
                a_high, a_low = attend[b, h]
                right_high = below(state_parts[0], fresh_parts[0])
                right_low = below(state_parts[1], fresh_parts[1])
                left_high = beside(q_high, a_high)
                left_low = beside(q_low, a_low)
                both = dot(left_high, right_high) + dot(left_low, right_high) + dot(left_high, right_low)
                at = pl.multiple_of(spot * BLOCK, BLOCK)
                out_ref[h, pl.ds(at, BLOCK), :] = both[:, :HEAD_DIM]
                r_high, r_low = split(both[:, HEAD_DIM:])
                reach_ref[h, pl.ds(at, BLOCK), :] = beside(r_high, r_low)
        return carry

    lax.fori_loop(0, count // per_step, step, 0)
    for h in range(share):
        final_ref[h] = state_ref[h]


def finish_kernel(dims, meta_ref, incoming_ref, gate_ref, gain_ref, *refs):
    share, gate_row, counts = dims
    out_ref, pieces = refs[-1], refs[:-1]
    piece_rows = BLOCK // 2
    is_first = meta_ref[meta_ref.shape[0] - 1]
    first_block = 0
    for number, count in enumerate(counts):
        core_ref, reach_ref = pieces[2 * number], pieces[2 * number + 1]

        def step(spot, carry, core_ref=core_ref, reach_ref=reach_ref, first_block=first_block):
            n = first_block + spot
            at = pl.multiple_of(spot * BLOCK, BLOCK)
            for h in range(share):
                high, low = split(jnp.where(is_first == 1, 0.0, incoming_ref[h]))
                row = beside(high, low)
                both = dot(reach_ref[h, pl.ds(at, BLOCK), :], below(row, row))
                core = core_ref[h, pl.ds(at, BLOCK), :] + both[:, :HEAD_DIM] + both[:, HEAD_DIM:]
                scale = lax.rsqrt(jnp.mean(core * core, axis=-1, keepdims=True) + 1e-06)
                gates = []
                for half in range(2):
                    place = meta_ref[2 * n + half]
                    start = gate_row + h * BLOCK + (place % 2) * piece_rows
                    start = pl.multiple_of(start, piece_rows)
                    gates.append(gate_ref[place // 2, pl.ds(start, piece_rows), :].astype(F32))
                gate = below(*gates)
                result = core * scale * gain_ref[...] * silu(gate)
                out_ref[n, h * BLOCK : (h + 1) * BLOCK, :] = result.astype(BF16)
            return carry

        lax.fori_loop(0, count, step, 0)
        first_block = first_block + count


def gather_kernel(moves, logit_place, *refs):
    sources = refs[: len(refs) - 2 - (1 if logit_place else 0)]
    if logit_place:
        first_row, heads = logit_place
        sources, logit_ref = sources[:-1], sources[-1]
        out_ref, sems, wide_ref = refs[-3], refs[-2], refs[-1]
    else:
        out_ref, sems = refs[-2], refs[-1]
    copies = []
    for number, (begin, length, column, place, row) in enumerate(moves):
        copies.append(
            pltpu.make_async_copy(
                sources[0].at[pl.ds(begin, length), pl.ds(column, HEAD_DIM)],
                out_ref.at[place, pl.ds(row, length), :],
                sems.at[number],
            )
        )
    for copy in copies:
        copy.start()
    if logit_place:
        tokens = logit_ref.shape[0]
        half = tokens // 2
        turned = logit_ref[...].astype(F32).T
        wide_ref[...] = jnp.zeros(wide_ref.shape, F32)
        wide_ref[0 : 2 * VALUE_HEADS, :] = turned
        lane = lax.broadcasted_iota(jnp.int32, (8, tokens), 1)
        for place in range(out_ref.shape[0]):
            early, late = [], []
            for kind in range(2):
                begin = kind * VALUE_HEADS + place * heads
                part = wide_ref[begin : begin + 8, :]
                rolled = pltpu.roll(part, half, 1)
                early.append(jnp.where(lane < half, part, rolled))
                late.append(jnp.where(lane < half, rolled, part))
            joined = below(*(early + late)).astype(BF16)
            out_ref[place, first_row : first_row + 32, :] = joined
    for copy in copies:
        copy.wait()


def scatter_kernel(moves, aliased, *refs):
    source_ref, out_ref, sems = refs[0], refs[-2], refs[-1]
    copies = []
    for number, (place, row, length, column) in enumerate(moves):
        copies.append(
            pltpu.make_async_copy(
                source_ref.at[place, pl.ds(row, length), :],
                out_ref.at[:, pl.ds(column, HEAD_DIM)],
                sems.at[number],
            )
        )
    for copy in copies:
        copy.start()
    for copy in copies:
        copy.wait()


MIB = 2**20


def limits(mib):
    return pltpu.CompilerParams(vmem_limit_bytes=mib * MIB)


def cost(flops):
    return pl.CostEstimate(flops=int(flops), bytes_accessed=2**20, transcendentals=0)


vmem = pl.BlockSpec(memory_space=pltpu.VMEM)
smem = pl.BlockSpec(memory_space=pltpu.SMEM)
anywhere = pl.BlockSpec(memory_space=pl.ANY)


def gather(name, source, moves, places, rows, logits=None, first_row=0, heads=0):
    operands, in_specs = [source], [anywhere]
    scratch = [pltpu.SemaphoreType.DMA((len(moves),))]
    logit_place = None
    if logits is not None:
        operands.append(logits)
        in_specs.append(vmem)
        scratch.append(pltpu.VMEM((2 * VALUE_HEADS + 8, logits.shape[0]), F32))
        logit_place = (first_row, heads)
    return pl.pallas_call(
        functools.partial(gather_kernel, tuple(moves), logit_place),
        out_shape=jax.ShapeDtypeStruct((places, rows, HEAD_DIM), BF16),
        in_specs=in_specs,
        out_specs=vmem,
        scratch_shapes=scratch,
        compiler_params=limits(6),
        cost_estimate=cost(8e8),
        name=name,
    )(*operands)


def scatter(name, source, moves, out_shape, base=None):
    operands, in_specs, aliases = [source], [vmem], {}
    if base is not None:
        operands.append(base)
        in_specs.append(anywhere)
        aliases = {1: 0}
    return pl.pallas_call(
        functools.partial(scatter_kernel, tuple(moves), base is not None),
        out_shape=jax.ShapeDtypeStruct(out_shape, BF16),
        in_specs=in_specs,
        out_specs=anywhere,
        scratch_shapes=[pltpu.SemaphoreType.DMA((len(moves),))],
        input_output_aliases=aliases,
        compiler_params=limits(4),
        cost_estimate=cost(8e8),
        name=name,
    )(*operands)


def passed_round(value, axis):
    length = lax.axis_size(axis)
    return lax.ppermute(value, axis, [(i, (i + 1) % length) for i in range(length)])


def exchanged(value):
    return lax.all_to_all(value, "cp", split_axis=0, concat_axis=0, tiled=True)


def per_device(mixed_qkv, gate_z, gate_logits, block_table, conv_weight, a_log, dt_bias, norm_gain):
    cp_count = lax.axis_size("cp")
    seg_count = lax.axis_size("seg")
    cp_place = lax.axis_index("cp")
    rows = mixed_qkv.shape[0]
    heads = VALUE_HEADS // cp_count
    groups = max(1, heads // GROUP)
    share = heads // groups
    tiles = 2 + share
    key_width = KEY_HEADS * HEAD_DIM
    count = cp_count * rows // BLOCK
    gate_row = tiles * BLOCK

    order = jnp.argsort(block_table[0]).astype(jnp.int32)
    is_first = (lax.axis_index("seg") == 0).astype(jnp.int32).reshape(1)
    meta = jnp.concatenate([order, is_first])

    def columns(place, group):
        value_head = place * heads + group * share
        key_head = value_head // GROUP
        found = [key_head * HEAD_DIM, key_width + key_head * HEAD_DIM]
        return found + [2 * key_width + (value_head + h) * HEAD_DIM for h in range(share)]

    def group_moves(group):
        return [
            (0, rows, column, place, tile * rows)
            for place in range(cp_count)
            for tile, column in enumerate(columns(place, group))
        ]

    received = []
    for group in range(groups):
        with_logits = dict(logits=gate_logits, first_row=gate_row, heads=heads) if group == 0 else {}
        sent = gather(
            "pack%d" % group,
            mixed_qkv,
            group_moves(group),
            cp_count,
            gate_row + (32 if group == 0 else 0),
            **with_logits,
        )
        received.append(exchanged(sent))
    tail_moves = [
        (rows - 16, 16, column, place, (group * tiles + tile) * 16)
        for place in range(cp_count)
        for group in range(groups)
        for tile, column in enumerate(columns(place, group))
    ]
    tails = gather("packtail", mixed_qkv, tail_moves, cp_count, groups * tiles * 16)
    tails = exchanged(tails)
    last = order[2 * cp_count - 1]
    tail = lax.dynamic_index_in_dim(tails, last // 2, 0, keepdims=False)
    tail = passed_round(tail, "seg").reshape(groups, tiles, 16, HEAD_DIM)

    gate_moves = [
        (0, rows, (place * heads + h) * HEAD_DIM, place, h * rows)
        for place in range(cp_count)
        for h in range(heads)
    ]
    gate_seq = exchanged(gather("packz", gate_z, gate_moves, cp_count, heads * rows))

    def group_weights(group):
        value_head = cp_place * heads + group * share
        key_head = value_head // GROUP
        shaped = conv_weight.reshape(CONV, -1, HEAD_DIM)
        picked = [
            lax.dynamic_slice_in_dim(shaped, key_head, 1, 1),
            lax.dynamic_slice_in_dim(shaped, KEY_HEADS + key_head, 1, 1),
            lax.dynamic_slice_in_dim(shaped, 2 * KEY_HEADS + value_head, share, 1),
        ]
        return jnp.concatenate(picked, axis=1).transpose(1, 0, 2)

    head_log = lax.dynamic_slice_in_dim(a_log, cp_place * heads, heads, 0)
    head_bias = lax.dynamic_slice_in_dim(dt_bias, cp_place * heads, heads, 0)
    rates = jnp.pad(jnp.stack([head_log, head_bias]), ((0, 0), (0, 8 - heads)))
    rates = jnp.broadcast_to(rates[:, :, None], (2, 8, BLOCK))

    def local(group, part, first_block, blocks, state):
        per_step = min(4, blocks)
        operands = [meta, received[group], received[0], tail[group], group_weights(group), rates]
        if state is not None:
            operands.append(state)
        in_specs = [smem] + [vmem] * (len(operands) - 1)
        dims = (group, share, first_block, blocks, per_step, gate_row, state is not None)
        return pl.pallas_call(
            functools.partial(local_kernel, dims),
            out_shape=(
                jax.ShapeDtypeStruct((share, blocks * BLOCK, HEAD_DIM), F32),
                jax.ShapeDtypeStruct((share, blocks * BLOCK, 2 * HEAD_DIM), BF16),
                jax.ShapeDtypeStruct((share, HEAD_DIM, 2 * HEAD_DIM), F32),
            ),
            in_specs=in_specs,
            out_specs=(vmem, vmem, vmem),
            scratch_shapes=[
                pltpu.VMEM((per_step * tiles, 8 + BLOCK, HEAD_DIM), F32),
                pltpu.VMEM((len(LEVELS), BLOCK, BLOCK), BF16),
                pltpu.VMEM((share, HEAD_DIM, 2 * HEAD_DIM), F32),
            ],
            compiler_params=limits(20),
            cost_estimate=cost(6e8 * blocks * share),
            name="local%d_%d" % (group, part),
        )(*operands)

    def chain(final):
        shift = final[:, :, :HEAD_DIM]
        reach_map = final[:, :, HEAD_DIM:]
        reach_map = jnp.where(lax.axis_index("seg") == 0, 0.0, reach_map)
        incoming = jnp.zeros((share, HEAD_DIM, HEAD_DIM), F32)
        for rounds in range(seg_count - 1):
            advanced = shift
            if rounds:
                advanced = shift + jnp.einsum(
                    "hij,hjk->hik", reach_map, incoming, precision=highest
                )
            incoming = passed_round(advanced, "seg")
        return incoming

    def finish(group, incoming, pieces, counts):
        flat = [array for piece in pieces for array in piece]
        return pl.pallas_call(
            functools.partial(finish_kernel, (share, group * share * rows, counts)),
            out_shape=jax.ShapeDtypeStruct((count, share * BLOCK, HEAD_DIM), BF16),
            in_specs=[smem] + [vmem] * (3 + len(flat)),
            out_specs=vmem,
            compiler_params=limits(8),
            cost_estimate=cost(1e9),
            name="finish%d" % group,
        )(meta, incoming, gate_seq, norm_gain.reshape(1, HEAD_DIM), *flat)

    result = None
    for group in range(groups):
        parts = 2 if group == 1 and count % 8 == 0 else 1
        state, pieces = None, []
        for part in range(parts):
            blocks = count // parts
            core, reach, state = local(group, part, part * blocks, blocks, state)
            pieces.append((core, reach))
        incoming = chain(state)
        done = finish(group, incoming, pieces, [count // parts] * parts)
        swapped = exchanged(done)
        moves = [
            (place, h * rows, rows, (place * heads + group * share + h) * HEAD_DIM)
            for place in range(cp_count)
            for h in range(share)
        ]
        result = scatter(
            "unpack%d" % group, swapped, moves, (rows, VALUE_HEADS * HEAD_DIM), result
        )
    return result


def solution(mesh):
    return jax.shard_map(
        per_device,
        mesh=mesh,
        in_specs=(
            P(("seg", "cp"), None),
            P(("seg", "cp"), None),
            P(("seg", "cp"), None),
            P("seg", None),
            P(),
            P(),
            P(),
            P(),
        ),
        out_specs=P(("seg", "cp"), None),
        check_vma=False,
    )
```

```python
import functools

import jax
import jax.numpy as jnp
from jax import lax
from jax.experimental import pallas as pl
from jax.experimental.pallas import tpu as pltpu
from jax.sharding import PartitionSpec as P


VALUE_HEADS = 32
KEY_HEADS = 16
HEAD_DIM = 128
CONV = 4
BLOCK = 128
GROUP = VALUE_HEADS // KEY_HEADS
LEVELS = (2, 4, 8, 16, 32, 64)

F32 = jnp.float32
BF16 = jnp.bfloat16


def dot(a, b):
    return jnp.dot(a, b, preferred_element_type=F32)


def split(x):
    high = x.astype(BF16)
    low = (x - high.astype(F32)).astype(BF16)
    return high, low


def beside(*parts):
    return jnp.concatenate(parts, axis=1)


def below(*parts):
    return jnp.concatenate(parts, axis=0)


def narrow_product(a, b):
    row = beside(b[0], b[1])
    both = dot(beside(a[0], a[1]), below(row, row))
    half = row.shape[1] // 2
    return both[:, :half] + both[:, half:]


def wide_product(a, b):
    return dot(beside(a[0], a[1]), below(b[0], b[0])) + dot(a[0], b[1])


def silu(v):
    return v / (1.0 + jnp.exp(-v))


def softplus(v):
    e = jnp.exp(-jnp.abs(v))
    s = e / (2.0 + e)
    t = s * s
    series = 1.0 / 19.0
    for odd in (17, 15, 13, 11, 9, 7, 5, 3, 1):
        series = series * t + 1.0 / odd
    return jnp.maximum(v, 0.0) + 2.0 * s * series


def together(*streams):
    alive = list(streams)
    while alive:
        for stream in list(alive):
            if next(stream, "over") == "over":
                alive.remove(stream)


def shifted_rows(meta_ref, recv_ref, rows_ref, slot, lead, n, first_row):
    piece_rows = BLOCK // 2
    place = meta_ref[jnp.maximum(2 * n - 1, 0)]
    start = first_row + (place % 2) * piece_rows + piece_rows - 16
    old = recv_ref[place // 2, pl.ds(pl.multiple_of(start, 16), 16), :].astype(F32)
    rows_ref[slot, 0:8, :] = jnp.where(n == 0, lead, old)[8:16]
    for half in range(2):
        place = meta_ref[2 * n + half]
        start = pl.multiple_of(first_row + (place % 2) * piece_rows, piece_rows)
        fresh = recv_ref[place // 2, pl.ds(start, piece_rows), :]
        begin = 8 + half * piece_rows
        rows_ref[slot, begin : begin + piece_rows, :] = fresh.astype(F32)


def convolved(rows_ref, slot, weight_ref, tile):
    summed = None
    for offset in range(CONV):
        begin = 8 - CONV + 1 + offset
        term = weight_ref[tile, offset : offset + 1, :] * rows_ref[slot, begin : begin + BLOCK, :]
        summed = term if summed is None else summed + term
    return silu(summed)


def unit_scale(matrix):
    return lax.rsqrt(jnp.sum(matrix * matrix, axis=-1, keepdims=True) + 1e-06)


def inner_kernel(
    dims,
    meta_ref,
    recv_ref,
    tail_ref,
    weight_ref,
    rate_ref,
    solved_out,
    state_out,
    flip_out,
    row_out,
    shift_ref,
    map_ref,
    solved_ref,
    before_ref,
    flip_ref,
    rows_ref,
    mask_ref,
    state_ref,
    sems,
):
    group, share, count, per_step, per_chunk = dims
    tiles = 1 + share
    gate_row = tiles * BLOCK
    piece_rows = BLOCK // 2
    is_first = meta_ref[meta_ref.shape[0] - 1]

    row_index = lax.broadcasted_iota(jnp.int32, (BLOCK, BLOCK), 0)
    col_index = lax.broadcasted_iota(jnp.int32, (BLOCK, BLOCK), 1)
    differ = row_index ^ col_index
    for place, size in enumerate(LEVELS):
        inside = (differ >= size) & (differ < 2 * size)
        mask_ref[place] = jnp.where(inside, 1.0, 0.0).astype(BF16)
    eye = jnp.where(row_index == col_index, 1.0, 0.0).astype(F32)
    strict = row_index > col_index
    upper = jnp.where(row_index <= col_index, 1.0, 0.0).astype(BF16)
    nothing = jnp.zeros((BLOCK, HEAD_DIM), F32)
    for h in range(share):
        state_ref[h] = beside(nothing, eye)

    def leaving(kind, n):
        at = pl.ds(pl.multiple_of(n * BLOCK, BLOCK), BLOCK)
        source, target = ((solved_ref, solved_out), (before_ref, state_out))[kind]
        return pltpu.make_async_copy(source.at[:, at, :], target.at[:, at, :], sems.at[kind, n])

    def leaving_flip(n):
        return pltpu.make_async_copy(flip_ref.at[n], flip_out.at[n], sems.at[2, n])

    def chunk(number, carry):
        steps = []
        for step in range(per_chunk // per_step):
            blocks = [number * per_chunk + step * per_step + b for b in range(per_step)]
            steps.append(dict(blocks=blocks, slot=step * per_step * tiles))

        def prepare(work):
            blocks = work["blocks"]
            lane = lax.broadcasted_iota(jnp.int32, (16, BLOCK), 1)
            work["line"], work["beta"], work["end"], work["keys"], work["values"] = {}, {}, {}, {}, {}
            work["system"], work["inverse"], work["grow"] = {}, {}, {}
            for b, n in enumerate(blocks):
                picked = []
                for half in range(2):
                    place = meta_ref[2 * n + half]
                    found = recv_ref[place // 2, gate_row : gate_row + 16, :].astype(F32)
                    turned = pltpu.roll(found, piece_rows, 1)
                    picked.append(jnp.where(place % 2 == half, found, turned))
                logits = jnp.where(lane < piece_rows, picked[0], picked[1])
                beta = 1.0 / (1.0 + jnp.exp(-logits[0:8]))
                decay = -jnp.exp(rate_ref[0]) * softplus(logits[8:16] + rate_ref[1])
                high = decay.astype(BF16)
                remain = decay - high.astype(F32)
                middle = remain.astype(BF16)
                low = (remain - middle.astype(F32)).astype(BF16)
                stacked = below(high.astype(F32), middle.astype(F32), low.astype(F32))
                stacked = below(stacked, jnp.zeros((8, BLOCK), F32)).astype(BF16)
                sums = dot(stacked, upper)
                cum = sums[0:8] + sums[8:16] + sums[16:24]
                row_out[0, n] = cum
                row_out[1, n] = beta
                work["line"][b], work["beta"][b] = cum, beta
                work["end"][b] = jnp.broadcast_to(cum[:, BLOCK - 1 :], (8, BLOCK))
                yield
            for b, n in enumerate(blocks):
                for tile in range(tiles):
                    slot = work["slot"] + b * tiles + tile
                    lead = jnp.where(is_first == 1, 0.0, tail_ref[tile].astype(F32))
                    shifted_rows(meta_ref, recv_ref, rows_ref, slot, lead, n, tile * BLOCK)
                    active = convolved(rows_ref, slot, weight_ref, tile)
                    if tile == 0:
                        work["keys"][b] = active * unit_scale(active)
                    else:
                        work["values"][b, tile - 1] = active
                    yield
                turned = work["keys"][b].T
                flip_ref[n] = turned
                leaving_flip(n).start()
                gram = narrow_product(split(work["keys"][b]), split(turned))
                yield
                columns = below(work["line"][b], jnp.zeros((BLOCK - 8, BLOCK), F32)).T
                for h in range(share):
                    at = group * share + h
                    column = jnp.broadcast_to(columns[:, at : at + 1], (BLOCK, BLOCK))
                    decay = jnp.exp(jnp.where(strict, column - work["line"][b][at : at + 1], 0.0))
                    work["grow"][b, h] = jnp.exp(column)
                    scaled = decay * work["beta"][b][at : at + 1]
                    lower = jnp.where(strict, gram * scaled, 0.0)
                    work["system"][b, h] = split(lower)
                    work["inverse"][b, h] = eye - jnp.where(differ == 1, lower, 0.0)
                    yield

        def invert(work):
            inverse, system = work["inverse"], work["system"]
            for place, size in enumerate(LEVELS):
                mask = mask_ref[place]
                halves, cross = {}, {}
                for u in inverse:
                    halves[u] = split(inverse[u])
                    parts = (system[u][0] * mask, system[u][1] * mask)
                    cross[u] = split(narrow_product(parts, halves[u]))
                    yield
                for u in inverse:
                    inverse[u] = inverse[u] - narrow_product(halves[u], cross[u])
                    yield

        def advance(work):
            blocks = work["blocks"]
            solved, shift, over, keep = {}, {}, {}, {}
            for b, n in enumerate(blocks):
                at = pl.ds(pl.multiple_of(n * BLOCK, BLOCK), BLOCK)
                for h in range(share):
                    row = group * share + h
                    right = split(beside(work["values"][b, h], work["keys"][b] * work["grow"][b, h]))
                    found = wide_product(split(work["inverse"][b, h]), right)
                    solved_ref[h, at, :] = found
                    solved[b, h] = split(found)
                    yield
                leaving(0, n).start()
            for b, n in enumerate(blocks):
                for h in range(share):
                    row = group * share + h
                    end, line = work["end"][b][row : row + 1], work["line"][b][row : row + 1]
                    weight = jnp.exp(end - line) * work["beta"][b][row : row + 1]
                    moved = wide_product(split(flip_ref[n] * weight), solved[b, h])
                    shift[b, h] = moved[:, :HEAD_DIM]
                    over[b, h] = split(moved[:, HEAD_DIM:])
                    keep[b, h] = beside(jnp.exp(end), jnp.exp(end))
                    yield
            for b, n in enumerate(blocks):
                at = pl.ds(pl.multiple_of(n * BLOCK, BLOCK), BLOCK)
                for h in range(share):
                    state = state_ref[h]
                    before_ref[h, at, :] = state
                    moved = wide_product(over[b, h], split(state))
                    state_ref[h] = state * keep[b, h] + beside(shift[b, h], nothing) - moved
                    yield
                leaving(1, n).start()

        together(prepare(steps[0]))
        for place, work in enumerate(steps):
            streams = [invert(work)]
            if place + 1 < len(steps):
                streams.append(prepare(steps[place + 1]))
            if place:
                streams.append(advance(steps[place - 1]))
            together(*streams)
        together(advance(steps[-1]))
        return carry

    if count == per_chunk:
        chunk(0, 0)
    else:
        lax.fori_loop(0, count // per_chunk, chunk, 0)
    for h in range(share):
        shift_ref[h] = state_ref[h, :, :HEAD_DIM]
        over = jnp.where(is_first == 1, 0.0, state_ref[h, :, HEAD_DIM:])
        map_high, map_low = split(over)
        map_ref[h] = beside(map_high, map_low)

    def drain(n, carry):
        leaving(0, n).wait()
        leaving(1, n).wait()
        leaving_flip(n).wait()
        return carry

    lax.fori_loop(0, count, drain, 0)


def advance_kernel(shift_ref, map_ref, incoming_ref, out_ref):
    for h in range(shift_ref.shape[0]):
        high, low = split(incoming_ref[h])
        row = beside(high, low)
        both = dot(map_ref[h], below(row, row))
        out_ref[h] = shift_ref[h] + both[:, :HEAD_DIM] + both[:, HEAD_DIM:]


def finish_kernel(
    dims,
    meta_ref,
    recv_ref,
    tail_ref,
    weight_ref,
    row_ref,
    incoming_ref,
    gain_ref,
    solved_in,
    state_in,
    flip_in,
    out_ref,
    solved_ref,
    before_ref,
    flip_ref,
    rows_ref,
    sems,
):
    group, share, count, per_step, query_row, gate_row = dims
    piece_rows = BLOCK // 2
    is_first = meta_ref[meta_ref.shape[0] - 1]
    row_index = lax.broadcasted_iota(jnp.int32, (BLOCK, BLOCK), 0)
    col_index = lax.broadcasted_iota(jnp.int32, (BLOCK, BLOCK), 1)
    inclusive = row_index >= col_index

    def arriving(n):
        at = pl.ds(pl.multiple_of(n * BLOCK, BLOCK), BLOCK)
        return (
            pltpu.make_async_copy(flip_in.at[n], flip_ref.at[n], sems.at[0, n]),
            pltpu.make_async_copy(state_in.at[:, at, :], before_ref.at[:, at, :], sems.at[1, n]),
            pltpu.make_async_copy(solved_in.at[:, at, :], solved_ref.at[:, at, :], sems.at[2, n]),
        )

    def fetch(n, carry):
        for copy in arriving(n):
            copy.start()
        return carry

    lax.fori_loop(0, count, fetch, 0)
    entry = [split(jnp.where(is_first == 1, 0.0, incoming_ref[h])) for h in range(share)]

    def step(index, carry):
        blocks = [index * per_step + b for b in range(per_step)]
        queries, grams = {}, {}
        for b, n in enumerate(blocks):
            lead = jnp.where(is_first == 1, 0.0, tail_ref[0].astype(F32))
            shifted_rows(meta_ref, recv_ref, rows_ref, b, lead, n, query_row)
            active = convolved(rows_ref, b, weight_ref, 0)
            queries[b] = active * (unit_scale(active) * HEAD_DIM ** (-0.5))
        for n in blocks:
            for copy in arriving(n):
                copy.wait()
        for b, n in enumerate(blocks):
            grams[b] = narrow_product(split(queries[b]), split(flip_ref[n]))
        units = [(b, h) for b in range(per_step) for h in range(share)]
        lefts, states, fresh = {}, {}, {}
        for b, h in units:
            n = blocks[b]
            at = group * share + h
            cum, beta = row_ref[0, n], row_ref[1, n]
            columns = below(cum, jnp.zeros((BLOCK - 8, BLOCK), F32)).T
            column = jnp.broadcast_to(columns[:, at : at + 1], (BLOCK, BLOCK))
            decay = jnp.exp(jnp.where(inclusive, column - cum[at : at + 1], 0.0))
            attend = jnp.where(inclusive, grams[b] * decay * beta[at : at + 1], 0.0)
            q_high, q_low = split(queries[b] * jnp.exp(column))
            a_high, a_low = split(attend)
            lefts[b, h] = (beside(q_high, a_high), beside(q_low, a_low))
        for b, h in units:
            rows = pl.ds(pl.multiple_of(blocks[b] * BLOCK, BLOCK), BLOCK)
            shift = before_ref[h, rows, :HEAD_DIM]
            over = split(before_ref[h, rows, HEAD_DIM:])
            states[b, h] = split(shift + narrow_product(over, entry[h]))
        for b, h in units:
            rows = pl.ds(pl.multiple_of(blocks[b] * BLOCK, BLOCK), BLOCK)
            px = split(solved_ref[h, rows, HEAD_DIM:])
            ux = solved_ref[h, rows, :HEAD_DIM]
            fresh[b, h] = split(ux - narrow_product(px, states[b, h]))
        for b, h in units:
            n = blocks[b]
            right = below(beside(*states[b, h]), beside(*fresh[b, h]))
            both = dot(lefts[b, h][0], right) + dot(lefts[b, h][1], right)
            core = both[:, :HEAD_DIM] + both[:, HEAD_DIM:]
            scale = lax.rsqrt(jnp.mean(core * core, axis=-1, keepdims=True) + 1e-06)
            gates = []
            for half in range(2):
                place = meta_ref[2 * n + half]
                start = gate_row + h * BLOCK + (place % 2) * piece_rows
                start = pl.multiple_of(start, piece_rows)
                gates.append(recv_ref[place // 2, pl.ds(start, piece_rows), :].astype(F32))
            gate = below(*gates)
            result = core * scale * gain_ref[...] * silu(gate)
            out_ref[n, h * BLOCK : (h + 1) * BLOCK, :] = result.astype(BF16)
        return carry

    lax.fori_loop(0, count // per_step, step, 0)


def gather_kernel(moves, source_count, logit_place, *refs):
    sources, refs = refs[:source_count], refs[source_count:]
    if logit_place:
        logit_ref, out_ref, sems, wide_ref = refs
    else:
        out_ref, sems = refs
    copies = []
    for number, (source, begin, length, column, place, row) in enumerate(moves):
        copies.append(
            pltpu.make_async_copy(
                sources[source].at[pl.ds(begin, length), pl.ds(column, HEAD_DIM)],
                out_ref.at[place, pl.ds(row, length), :],
                sems.at[number],
            )
        )
    for copy in copies:
        copy.start()
    if logit_place:
        first_row, heads = logit_place
        wide_ref[...] = jnp.zeros(wide_ref.shape, F32)
        wide_ref[0 : 2 * VALUE_HEADS, :] = logit_ref[...].astype(F32)
        for place in range(out_ref.shape[0]):
            begin = place * heads
            rates = wide_ref[begin : begin + 8, :]
            steps = wide_ref[VALUE_HEADS + begin : VALUE_HEADS + begin + 8, :]
            out_ref[place, first_row : first_row + 16, :] = below(rates, steps).astype(BF16)
    for copy in copies:
        copy.wait()


def halo_kernel(total, rows, meta_ref, arrived_ref, out_ref, sems):
    last = meta_ref[meta_ref.shape[0] - 2]
    copies = []
    for tile in range(total):
        source = arrived_ref.at[last // 2, pl.ds(tile * rows + rows - 16, 16), :]
        copies.append(pltpu.make_async_copy(source, out_ref.at[tile], sems.at[tile]))
    for copy in copies:
        copy.start()
    for copy in copies:
        copy.wait()


def scatter_kernel(moves, *refs):
    source_ref, out_ref, sems = refs[0], refs[-2], refs[-1]
    copies = []
    for number, (place, row, length, column) in enumerate(moves):
        copies.append(
            pltpu.make_async_copy(
                source_ref.at[place, pl.ds(row, length), :],
                out_ref.at[:, pl.ds(column, HEAD_DIM)],
                sems.at[number],
            )
        )
    for copy in copies:
        copy.start()
    for copy in copies:
        copy.wait()


MIB = 2**20
GATHER_MIB = 6
INNER_MIB = 24
FINISH_MIB = 20


def limits(mib):
    return pltpu.CompilerParams(vmem_limit_bytes=mib * MIB)


def cost(flops):
    return pl.CostEstimate(flops=int(flops), bytes_accessed=2**20, transcendentals=0)


vmem = pl.BlockSpec(memory_space=pltpu.VMEM)
smem = pl.BlockSpec(memory_space=pltpu.SMEM)
anywhere = pl.BlockSpec(memory_space=pl.ANY)
stored = pl.BlockSpec(memory_space=pltpu.HBM)


def gather(sources, moves, places, rows, logits=None, first_row=0, heads=0):
    operands, in_specs = list(sources), [anywhere] * len(sources)
    scratch = [pltpu.SemaphoreType.DMA((len(moves),))]
    logit_place = None
    if logits is not None:
        operands.append(logits)
        in_specs.append(vmem)
        scratch.append(pltpu.VMEM((2 * VALUE_HEADS + 8, logits.shape[1]), F32))
        logit_place = (first_row, heads)
    return pl.pallas_call(
        functools.partial(gather_kernel, tuple(moves), len(sources), logit_place),
        out_shape=jax.ShapeDtypeStruct((places, rows, HEAD_DIM), BF16),
        in_specs=in_specs,
        out_specs=vmem,
        scratch_shapes=scratch,
        compiler_params=limits(GATHER_MIB),
        cost_estimate=cost(8e8),
    )(*operands)


def scatter(source, moves, out_shape, base=None):
    operands, in_specs, aliases = [source], [vmem], {}
    if base is not None:
        operands.append(base)
        in_specs.append(anywhere)
        aliases = {1: 0}
    return pl.pallas_call(
        functools.partial(scatter_kernel, tuple(moves)),
        out_shape=jax.ShapeDtypeStruct(out_shape, BF16),
        in_specs=in_specs,
        out_specs=anywhere,
        scratch_shapes=[pltpu.SemaphoreType.DMA((len(moves),))],
        input_output_aliases=aliases,
        compiler_params=limits(4),
        cost_estimate=cost(8e8),
    )(*operands)


def passed_round(value, axis):
    length = lax.axis_size(axis)
    return lax.ppermute(value, axis, [(i, (i + 1) % length) for i in range(length)])


def exchanged(value):
    return lax.all_to_all(value, "cp", split_axis=0, concat_axis=0, tiled=True)


def per_device(mixed_qkv, gate_z, gate_logits, block_table, conv_weight, a_log, dt_bias, norm_gain):
    cp_count = lax.axis_size("cp")
    seg_count = lax.axis_size("seg")
    cp_place = lax.axis_index("cp")
    rows = mixed_qkv.shape[0]
    heads = VALUE_HEADS // cp_count
    groups = max(1, heads // GROUP)
    share = heads // groups
    tiles = 1 + share
    key_width = KEY_HEADS * HEAD_DIM
    count = cp_count * rows // BLOCK
    gate_row = tiles * BLOCK

    order = jnp.argsort(block_table[0]).astype(jnp.int32)
    is_first = (lax.axis_index("seg") == 0).astype(jnp.int32).reshape(1)
    meta = jnp.concatenate([order, is_first])

    def key_head(place, group):
        return (place * heads + group * share) // GROUP

    def inner_moves(group):
        moves = []
        for place in range(cp_count):
            found = [key_width + key_head(place, group) * HEAD_DIM]
            for h in range(share):
                found.append(2 * key_width + (place * heads + group * share + h) * HEAD_DIM)
            for tile, column in enumerate(found):
                moves.append((0, 0, rows, column, place, tile * rows))
        return moves

    def outer_moves():
        moves = []
        for place in range(cp_count):
            for group in range(groups):
                moves.append((0, 0, rows, key_head(place, group) * HEAD_DIM, place, group * rows))
            for h in range(heads):
                moves.append((1, 0, rows, (place * heads + h) * HEAD_DIM, place, (groups + h) * rows))
        return moves

    def halo(arrived, total):
        found = pl.pallas_call(
            functools.partial(halo_kernel, total, rows),
            out_shape=jax.ShapeDtypeStruct((total, 16, HEAD_DIM), BF16),
            in_specs=[smem, anywhere],
            out_specs=vmem,
            scratch_shapes=[pltpu.SemaphoreType.DMA((total,))],
            compiler_params=limits(2),
            cost_estimate=cost(1e8),
        )(meta, arrived)
        return passed_round(found, "seg")

    received, tails = [], []
    for group in range(groups):
        sent = gather(
            [mixed_qkv],
            inner_moves(group),
            cp_count,
            gate_row + 16,
            logits=gate_logits.T,
            first_row=gate_row,
            heads=heads,
        )
        received.append(exchanged(sent))
        tails.append(halo(received[group], tiles))

    packed = gather([mixed_qkv, gate_z], outer_moves(), cp_count, (groups + heads) * rows)
    outer = exchanged(packed)
    outer_tail = halo(outer, groups)

    shaped = conv_weight.reshape(CONV, -1, HEAD_DIM)

    def taps(first, total):
        return lax.dynamic_slice_in_dim(shaped, first, total, 1).transpose(1, 0, 2)

    weights, query_weights = [], []
    for group in range(groups):
        own_key = key_head(cp_place, group)
        own_value = 2 * KEY_HEADS + cp_place * heads + group * share
        query_weights.append(taps(own_key, 1))
        weights.append(
            jnp.concatenate([taps(KEY_HEADS + own_key, 1), taps(own_value, share)], axis=0)
        )
    head_log = lax.dynamic_slice_in_dim(a_log, cp_place * heads, heads, 0)
    head_bias = lax.dynamic_slice_in_dim(dt_bias, cp_place * heads, heads, 0)
    rates = jnp.pad(jnp.stack([head_log, head_bias]), ((0, 0), (0, 8 - heads)))
    rates = jnp.broadcast_to(rates[:, :, None], (2, 8, BLOCK))

    per_step = min(4, count)
    per_chunk = min(8, count)

    def inner(group):
        dims = (group, share, count, per_step, per_chunk)
        wide = (share, count * BLOCK, 2 * HEAD_DIM)
        return pl.pallas_call(
            functools.partial(inner_kernel, dims),
            out_shape=(
                pltpu.HBM(wide, F32),
                pltpu.HBM(wide, F32),
                pltpu.HBM((count, HEAD_DIM, BLOCK), F32),
                jax.ShapeDtypeStruct((2, count, 8, BLOCK), F32),
                jax.ShapeDtypeStruct((share, HEAD_DIM, HEAD_DIM), F32),
                jax.ShapeDtypeStruct((share, HEAD_DIM, 2 * HEAD_DIM), BF16),
            ),
            in_specs=[smem] + [vmem] * 4,
            out_specs=(stored, stored, stored, vmem, vmem, vmem),
            scratch_shapes=[
                pltpu.VMEM(wide, F32),
                pltpu.VMEM(wide, F32),
                pltpu.VMEM((count, HEAD_DIM, BLOCK), F32),
                pltpu.VMEM((per_chunk * tiles, 8 + BLOCK, HEAD_DIM), F32),
                pltpu.VMEM((len(LEVELS), BLOCK, BLOCK), BF16),
                pltpu.VMEM((share, HEAD_DIM, 2 * HEAD_DIM), F32),
                pltpu.SemaphoreType.DMA((3, count)),
            ],
            compiler_params=limits(INNER_MIB),
            cost_estimate=cost(6e8 * count * share),
        )(meta, received[group], tails[group], weights[group], rates)

    def chain(shift, over):
        incoming = None
        for rounds in range(seg_count - 1):
            advanced = shift
            if rounds:
                advanced = pl.pallas_call(
                    advance_kernel,
                    out_shape=jax.ShapeDtypeStruct(shift.shape, F32),
                    in_specs=[vmem] * 3,
                    out_specs=vmem,
                    compiler_params=limits(3),
                    cost_estimate=cost(2e8),
                )(shift, over, incoming)
            incoming = passed_round(advanced, "seg")
        if incoming is None:
            incoming = jnp.zeros_like(shift)
        return incoming

    def finish(group, incoming, solved, before, flip, lines):
        dims = (group, share, count, per_step, group * rows, (groups + group * share) * rows)
        wide = (share, count * BLOCK, 2 * HEAD_DIM)
        return pl.pallas_call(
            functools.partial(finish_kernel, dims),
            out_shape=jax.ShapeDtypeStruct((count, share * BLOCK, HEAD_DIM), BF16),
            in_specs=[smem] + [vmem] * 6 + [stored] * 3,
            out_specs=vmem,
            scratch_shapes=[
                pltpu.VMEM(wide, F32),
                pltpu.VMEM(wide, F32),
                pltpu.VMEM((count, HEAD_DIM, BLOCK), F32),
                pltpu.VMEM((per_step, 8 + BLOCK, HEAD_DIM), F32),
                pltpu.SemaphoreType.DMA((3, count)),
            ],
            compiler_params=limits(FINISH_MIB),
            cost_estimate=cost(1.5e9),
        )(
            meta,
            outer,
            outer_tail[group : group + 1],
            query_weights[group],
            lines,
            incoming,
            norm_gain.reshape(1, HEAD_DIM),
            *[pltpu.with_memory_space_constraint(x, pltpu.HBM) for x in (solved, before, flip)],
        )

    result = None
    for group in range(groups):
        solved, before, flip, lines, shift, over = inner(group)
        incoming = chain(shift, over)
        done = finish(group, incoming, solved, before, flip, lines)
        swapped = exchanged(done)
        moves = [
            (place, h * rows, rows, (place * heads + group * share + h) * HEAD_DIM)
            for place in range(cp_count)
            for h in range(share)
        ]
        result = scatter(swapped, moves, (rows, VALUE_HEADS * HEAD_DIM), result)
    return result


def solution(mesh):
    return jax.shard_map(
        per_device,
        mesh=mesh,
        in_specs=(
            P(("seg", "cp"), None),
            P(("seg", "cp"), None),
            P(("seg", "cp"), None),
            P("seg", None),
            P(),
            P(),
            P(),
            P(),
        ),
        out_specs=P(("seg", "cp"), None),
        check_vma=False,
    )
```

```python
import functools

import jax
import jax.numpy as jnp
from jax import lax
from jax.experimental import pallas as pl
from jax.experimental.pallas import tpu as pltpu
from jax.sharding import PartitionSpec as P


VALUE_HEADS = 32
KEY_HEADS = 16
HEAD_DIM = 128
CONV = 4
BLOCK = 128
GROUP = VALUE_HEADS // KEY_HEADS
LEVELS = (2, 4, 8, 16, 32, 64)

F32 = jnp.float32
BF16 = jnp.bfloat16


def dot(a, b):
    return jnp.dot(a, b, preferred_element_type=F32)


def split(x):
    high = x.astype(BF16)
    low = (x - high.astype(F32)).astype(BF16)
    return high, low


def beside(*parts):
    return jnp.concatenate(parts, axis=1)


def below(*parts):
    return jnp.concatenate(parts, axis=0)


def narrow_product(a, b):
    row = beside(b[0], b[1])
    both = dot(beside(a[0], a[1]), below(row, row))
    half = row.shape[1] // 2
    return both[:, :half] + both[:, half:]


def wide_product(a, b):
    return dot(beside(a[0], a[1]), below(b[0], b[0])) + dot(a[0], b[1])


def silu(v):
    return v / (1.0 + jnp.exp(-v))


def softplus(v):
    e = jnp.exp(-jnp.abs(v))
    s = e / (2.0 + e)
    t = s * s
    series = 1.0 / 19.0
    for odd in (17, 15, 13, 11, 9, 7, 5, 3, 1):
        series = series * t + 1.0 / odd
    return jnp.maximum(v, 0.0) + 2.0 * s * series


def together(*streams):
    alive = list(streams)
    while alive:
        for stream in list(alive):
            if next(stream, "over") == "over":
                alive.remove(stream)


def shifted_rows(meta_ref, recv_ref, rows_ref, slot, lead, n, first_row):
    piece_rows = BLOCK // 2
    place = meta_ref[jnp.maximum(2 * n - 1, 0)]
    start = first_row + (place % 2) * piece_rows + piece_rows - 16
    old = recv_ref[place // 2, pl.ds(pl.multiple_of(start, 16), 16), :].astype(F32)
    rows_ref[slot, 0:8, :] = jnp.where(n == 0, lead, old)[8:16]
    for half in range(2):
        place = meta_ref[2 * n + half]
        start = pl.multiple_of(first_row + (place % 2) * piece_rows, piece_rows)
        fresh = recv_ref[place // 2, pl.ds(start, piece_rows), :]
        begin = 8 + half * piece_rows
        rows_ref[slot, begin : begin + piece_rows, :] = fresh.astype(F32)


def convolved(rows_ref, slot, weight_ref, tile):
    summed = None
    for offset in range(CONV):
        begin = 8 - CONV + 1 + offset
        term = weight_ref[tile, offset : offset + 1, :] * rows_ref[slot, begin : begin + BLOCK, :]
        summed = term if summed is None else summed + term
    return silu(summed)


def unit_scale(matrix):
    return lax.rsqrt(jnp.sum(matrix * matrix, axis=-1, keepdims=True) + 1e-06)


def inner_kernel(dims, meta_ref, recv_ref, tail_ref, weight_ref, rate_ref, *refs):
    group, share, first_block, count, per_step, per_chunk, last_part = dims
    if first_block:
        given_ref = refs[0]
        refs = refs[4:]
    else:
        given_ref = None
    solved_out, state_out, flip_out, row_out, refs = *refs[:4], refs[4:]
    if last_part:
        shift_ref, map_ref, refs = *refs[:2], refs[2:]
    else:
        final_ref, refs = refs[0], refs[1:]
    solved_ref, before_ref, flip_ref, rows_ref, mask_ref, state_ref, sems = refs
    tiles = 1 + share
    gate_row = tiles * BLOCK
    piece_rows = BLOCK // 2
    is_first = meta_ref[meta_ref.shape[0] - 1]

    row_index = lax.broadcasted_iota(jnp.int32, (BLOCK, BLOCK), 0)
    col_index = lax.broadcasted_iota(jnp.int32, (BLOCK, BLOCK), 1)
    differ = row_index ^ col_index
    for place, size in enumerate(LEVELS):
        inside = (differ >= size) & (differ < 2 * size)
        mask_ref[place] = jnp.where(inside, 1.0, 0.0).astype(BF16)
    eye = jnp.where(row_index == col_index, 1.0, 0.0).astype(F32)
    strict = row_index > col_index
    upper = jnp.where(row_index <= col_index, 1.0, 0.0).astype(BF16)
    nothing = jnp.zeros((BLOCK, HEAD_DIM), F32)
    for h in range(share):
        state_ref[h] = beside(nothing, eye) if given_ref is None else given_ref[h]

    def leaving(kind, n):
        here = pl.ds(pl.multiple_of(n * BLOCK, BLOCK), BLOCK)
        there = pl.ds(pl.multiple_of((first_block + n) * BLOCK, BLOCK), BLOCK)
        source, target = ((solved_ref, solved_out), (before_ref, state_out))[kind]
        return pltpu.make_async_copy(source.at[:, here, :], target.at[:, there, :], sems.at[kind, n])

    def leaving_flip(n):
        return pltpu.make_async_copy(flip_ref.at[n], flip_out.at[first_block + n], sems.at[2, n])

    def chunk(number, carry):
        steps = []
        for step in range(per_chunk // per_step):
            blocks = [number * per_chunk + step * per_step + b for b in range(per_step)]
            steps.append(dict(blocks=blocks, slot=step * per_step * tiles))

        def prepare(work):
            blocks = work["blocks"]
            lane = lax.broadcasted_iota(jnp.int32, (16, BLOCK), 1)
            work["line"], work["beta"], work["end"], work["keys"], work["values"] = {}, {}, {}, {}, {}
            work["system"], work["inverse"], work["grow"] = {}, {}, {}
            for b, n in enumerate(blocks):
                picked = []
                for half in range(2):
                    place = meta_ref[2 * (first_block + n) + half]
                    found = recv_ref[place // 2, gate_row : gate_row + 16, :].astype(F32)
                    turned = pltpu.roll(found, piece_rows, 1)
                    picked.append(jnp.where(place % 2 == half, found, turned))
                logits = jnp.where(lane < piece_rows, picked[0], picked[1])
                beta = 1.0 / (1.0 + jnp.exp(-logits[0:8]))
                decay = -jnp.exp(rate_ref[0]) * softplus(logits[8:16] + rate_ref[1])
                high = decay.astype(BF16)
                remain = decay - high.astype(F32)
                middle = remain.astype(BF16)
                low = (remain - middle.astype(F32)).astype(BF16)
                stacked = below(high.astype(F32), middle.astype(F32), low.astype(F32))
                stacked = below(stacked, jnp.zeros((8, BLOCK), F32)).astype(BF16)
                sums = dot(stacked, upper)
                cum = sums[0:8] + sums[8:16] + sums[16:24]
                row_out[0, n] = cum
                row_out[1, n] = beta
                work["line"][b], work["beta"][b] = cum, beta
                work["end"][b] = jnp.broadcast_to(cum[:, BLOCK - 1 :], (8, BLOCK))
                yield
            for b, n in enumerate(blocks):
                for tile in range(tiles):
                    slot = work["slot"] + b * tiles + tile
                    lead = jnp.where(is_first == 1, 0.0, tail_ref[tile].astype(F32))
                    shifted_rows(meta_ref, recv_ref, rows_ref, slot, lead, first_block + n, tile * BLOCK)
                    active = convolved(rows_ref, slot, weight_ref, tile)
                    if tile == 0:
                        work["keys"][b] = active * unit_scale(active)
                    else:
                        work["values"][b, tile - 1] = active
                    yield
                turned = work["keys"][b].T
                flip_ref[n] = turned
                leaving_flip(n).start()
                gram = narrow_product(split(work["keys"][b]), split(turned))
                yield
                columns = below(work["line"][b], jnp.zeros((BLOCK - 8, BLOCK), F32)).T
                for h in range(share):
                    at = group * share + h
                    column = jnp.broadcast_to(columns[:, at : at + 1], (BLOCK, BLOCK))
                    decay = jnp.exp(jnp.where(strict, column - work["line"][b][at : at + 1], 0.0))
                    work["grow"][b, h] = jnp.exp(column)
                    scaled = decay * work["beta"][b][at : at + 1]
                    lower = jnp.where(strict, gram * scaled, 0.0)
                    work["system"][b, h] = split(lower)
                    work["inverse"][b, h] = eye - jnp.where(differ == 1, lower, 0.0)
                    yield

        def invert(work):
            inverse, system = work["inverse"], work["system"]
            for place, size in enumerate(LEVELS):
                mask = mask_ref[place]
                halves, cross = {}, {}
                for u in inverse:
                    halves[u] = split(inverse[u])
                    parts = (system[u][0] * mask, system[u][1] * mask)
                    cross[u] = split(narrow_product(parts, halves[u]))
                    yield
                for u in inverse:
                    inverse[u] = inverse[u] - narrow_product(halves[u], cross[u])
                    yield

        def advance(work):
            blocks = work["blocks"]
            solved, shift, over, keep = {}, {}, {}, {}
            for b, n in enumerate(blocks):
                at = pl.ds(pl.multiple_of(n * BLOCK, BLOCK), BLOCK)
                for h in range(share):
                    row = group * share + h
                    right = split(beside(work["values"][b, h], work["keys"][b] * work["grow"][b, h]))
                    found = wide_product(split(work["inverse"][b, h]), right)
                    solved_ref[h, at, :] = found
                    solved[b, h] = split(found)
                    yield
                leaving(0, n).start()
            for b, n in enumerate(blocks):
                for h in range(share):
                    row = group * share + h
                    end, line = work["end"][b][row : row + 1], work["line"][b][row : row + 1]
                    weight = jnp.exp(end - line) * work["beta"][b][row : row + 1]
                    moved = wide_product(split(flip_ref[n] * weight), solved[b, h])
                    shift[b, h] = moved[:, :HEAD_DIM]
                    over[b, h] = split(moved[:, HEAD_DIM:])
                    keep[b, h] = beside(jnp.exp(end), jnp.exp(end))
                    yield
            for b, n in enumerate(blocks):
                at = pl.ds(pl.multiple_of(n * BLOCK, BLOCK), BLOCK)
                for h in range(share):
                    state = state_ref[h]
                    before_ref[h, at, :] = state
                    moved = wide_product(over[b, h], split(state))
                    state_ref[h] = state * keep[b, h] + beside(shift[b, h], nothing) - moved
                    yield
                leaving(1, n).start()

        together(prepare(steps[0]))
        for place, work in enumerate(steps):
            streams = [invert(work)]
            if place + 1 < len(steps):
                streams.append(prepare(steps[place + 1]))
            if place:
                streams.append(advance(steps[place - 1]))
            together(*streams)
        together(advance(steps[-1]))
        return carry

    if count == per_chunk:
        chunk(0, 0)
    else:
        lax.fori_loop(0, count // per_chunk, chunk, 0)
    for h in range(share):
        if last_part:
            shift_ref[h] = state_ref[h, :, :HEAD_DIM]
            over = jnp.where(is_first == 1, 0.0, state_ref[h, :, HEAD_DIM:])
            map_high, map_low = split(over)
            map_ref[h] = beside(map_high, map_low)
        else:
            final_ref[h] = state_ref[h]

    def drain(n, carry):
        leaving(0, n).wait()
        leaving(1, n).wait()
        leaving_flip(n).wait()
        return carry

    lax.fori_loop(0, count, drain, 0)


def advance_kernel(shift_ref, map_ref, incoming_ref, out_ref):
    for h in range(shift_ref.shape[0]):
        high, low = split(incoming_ref[h])
        row = beside(high, low)
        both = dot(map_ref[h], below(row, row))
        out_ref[h] = shift_ref[h] + both[:, :HEAD_DIM] + both[:, HEAD_DIM:]


def finish_kernel(
    dims,
    meta_ref,
    outer_ref,
    tail_ref,
    weight_ref,
    incoming_ref,
    gain_ref,
    solved_in,
    state_in,
    flip_in,
    *refs,
):
    group, share, counts, query_row, gate_row, tail_place = dims
    count = sum(counts)
    line_refs = refs[: len(counts)]
    out_ref, solved_ref, before_ref, flip_ref, rows_ref, sems = refs[len(counts) :]
    piece_rows = BLOCK // 2
    is_first = meta_ref[meta_ref.shape[0] - 1]
    row_index = lax.broadcasted_iota(jnp.int32, (BLOCK, BLOCK), 0)
    col_index = lax.broadcasted_iota(jnp.int32, (BLOCK, BLOCK), 1)
    inclusive = row_index >= col_index

    def arriving(n):
        at = pl.ds(pl.multiple_of(n * BLOCK, BLOCK), BLOCK)
        return (
            pltpu.make_async_copy(flip_in.at[n], flip_ref.at[n], sems.at[0, n]),
            pltpu.make_async_copy(state_in.at[:, at, :], before_ref.at[:, at, :], sems.at[1, n]),
            pltpu.make_async_copy(solved_in.at[:, at, :], solved_ref.at[:, at, :], sems.at[2, n]),
        )

    def fetch(n, carry):
        for copy in arriving(n):
            copy.start()
        return carry

    lax.fori_loop(0, count, fetch, 0)
    entry = [split(jnp.where(is_first == 1, 0.0, incoming_ref[h])) for h in range(share)]

    def step(index, carry, first_block, per_step, row_ref):
        spots = [index * per_step + b for b in range(per_step)]
        blocks = [first_block + spot for spot in spots]
        queries, grams = {}, {}
        for b, n in enumerate(blocks):
            lead = jnp.where(is_first == 1, 0.0, tail_ref[tail_place].astype(F32))
            shifted_rows(meta_ref, outer_ref, rows_ref, b, lead, n, query_row)
            active = convolved(rows_ref, b, weight_ref, 0)
            queries[b] = active * (unit_scale(active) * HEAD_DIM ** (-0.5))
        for n in blocks:
            for copy in arriving(n):
                copy.wait()
        for b, n in enumerate(blocks):
            grams[b] = narrow_product(split(queries[b]), split(flip_ref[n]))
        units = [(b, h) for b in range(per_step) for h in range(share)]
        lefts, states, fresh = {}, {}, {}
        for b, h in units:
            n = blocks[b]
            at = group * share + h
            cum, beta = row_ref[0, spots[b]], row_ref[1, spots[b]]
            columns = below(cum, jnp.zeros((BLOCK - 8, BLOCK), F32)).T
            column = jnp.broadcast_to(columns[:, at : at + 1], (BLOCK, BLOCK))
            decay = jnp.exp(jnp.where(inclusive, column - cum[at : at + 1], 0.0))
            attend = jnp.where(inclusive, grams[b] * decay * beta[at : at + 1], 0.0)
            q_high, q_low = split(queries[b] * jnp.exp(column))
            a_high, a_low = split(attend)
            lefts[b, h] = (beside(q_high, a_high), beside(q_low, a_low))
        for b, h in units:
            rows = pl.ds(pl.multiple_of(blocks[b] * BLOCK, BLOCK), BLOCK)
            shift = before_ref[h, rows, :HEAD_DIM]
            over = split(before_ref[h, rows, HEAD_DIM:])
            states[b, h] = split(shift + narrow_product(over, entry[h]))
        for b, h in units:
            rows = pl.ds(pl.multiple_of(blocks[b] * BLOCK, BLOCK), BLOCK)
            px = split(solved_ref[h, rows, HEAD_DIM:])
            ux = solved_ref[h, rows, :HEAD_DIM]
            fresh[b, h] = split(ux - narrow_product(px, states[b, h]))
        for b, h in units:
            n = blocks[b]
            right = below(beside(*states[b, h]), beside(*fresh[b, h]))
            both = dot(lefts[b, h][0], right) + dot(lefts[b, h][1], right)
            core = both[:, :HEAD_DIM] + both[:, HEAD_DIM:]
            scale = lax.rsqrt(jnp.mean(core * core, axis=-1, keepdims=True) + 1e-06)
            gates = []
            for half in range(2):
                place = meta_ref[2 * n + half]
                start = gate_row + h * BLOCK + (place % 2) * piece_rows
                start = pl.multiple_of(start, piece_rows)
                gates.append(outer_ref[place // 2, pl.ds(start, piece_rows), :].astype(F32))
            gate = below(*gates)
            result = core * scale * gain_ref[...] * silu(gate)
            out_ref[n, h * BLOCK : (h + 1) * BLOCK, :] = result.astype(BF16)
        return carry

    first_block = 0
    for blocks, row_ref in zip(counts, line_refs):
        per_step = min(4, blocks)
        part = functools.partial(step, first_block=first_block, per_step=per_step, row_ref=row_ref)
        if blocks == per_step:
            part(0, 0)
        else:
            lax.fori_loop(0, blocks // per_step, part, 0)
        first_block += blocks


def gather_kernel(moves, source_count, logit_place, *refs):
    sources, refs = refs[:source_count], refs[source_count:]
    if logit_place:
        logit_ref, out_ref, sems, wide_ref = refs
    else:
        out_ref, sems = refs
    copies = []
    for number, (source, begin, length, column, place, row) in enumerate(moves):
        copies.append(
            pltpu.make_async_copy(
                sources[source].at[pl.ds(begin, length), pl.ds(column, HEAD_DIM)],
                out_ref.at[place, pl.ds(row, length), :],
                sems.at[number],
            )
        )
    for copy in copies:
        copy.start()
    if logit_place:
        first_row, heads = logit_place
        wide_ref[...] = jnp.zeros(wide_ref.shape, F32)
        wide_ref[0 : 2 * VALUE_HEADS, :] = logit_ref[...].astype(F32)
        for place in range(out_ref.shape[0]):
            begin = place * heads
            rates = wide_ref[begin : begin + 8, :]
            steps = wide_ref[VALUE_HEADS + begin : VALUE_HEADS + begin + 8, :]
            out_ref[place, first_row : first_row + 16, :] = below(rates, steps).astype(BF16)
    for copy in copies:
        copy.wait()


def halo_kernel(places, meta_ref, arrived_ref, out_ref, sems):
    last = meta_ref[meta_ref.shape[0] - 2]
    copies = []
    for tile, row in enumerate(places):
        source = arrived_ref.at[last // 2, pl.ds(row, 16), :]
        copies.append(pltpu.make_async_copy(source, out_ref.at[tile], sems.at[tile]))
    for copy in copies:
        copy.start()
    for copy in copies:
        copy.wait()


def scatter_kernel(moves, *refs):
    source_ref, out_ref, sems = refs[0], refs[-2], refs[-1]
    copies = []
    for number, (place, row, length, column) in enumerate(moves):
        copies.append(
            pltpu.make_async_copy(
                source_ref.at[place, pl.ds(row, length), :],
                out_ref.at[:, pl.ds(column, HEAD_DIM)],
                sems.at[number],
            )
        )
    for copy in copies:
        copy.start()
    for copy in copies:
        copy.wait()


MIB = 2**20
GATHER_MIB = 6
INNER_MIB = 24
FINISH_MIB = 20


def limits(mib):
    return pltpu.CompilerParams(vmem_limit_bytes=mib * MIB)


def cost(flops):
    return pl.CostEstimate(flops=int(flops), bytes_accessed=2**20, transcendentals=0)


vmem = pl.BlockSpec(memory_space=pltpu.VMEM)
smem = pl.BlockSpec(memory_space=pltpu.SMEM)
anywhere = pl.BlockSpec(memory_space=pl.ANY)
stored = pl.BlockSpec(memory_space=pltpu.HBM)


def gather(sources, moves, places, rows, logits=None, first_row=0, heads=0):
    operands, in_specs = list(sources), [anywhere] * len(sources)
    scratch = [pltpu.SemaphoreType.DMA((len(moves),))]
    logit_place = None
    if logits is not None:
        operands.append(logits)
        in_specs.append(vmem)
        scratch.append(pltpu.VMEM((2 * VALUE_HEADS + 8, logits.shape[1]), F32))
        logit_place = (first_row, heads)
    return pl.pallas_call(
        functools.partial(gather_kernel, tuple(moves), len(sources), logit_place),
        out_shape=jax.ShapeDtypeStruct((places, rows, HEAD_DIM), BF16),
        in_specs=in_specs,
        out_specs=vmem,
        scratch_shapes=scratch,
        compiler_params=limits(GATHER_MIB),
        cost_estimate=cost(8e8),
    )(*operands)


def scatter(source, moves, out_shape, base=None):
    operands, in_specs, aliases = [source], [vmem], {}
    if base is not None:
        operands.append(base)
        in_specs.append(anywhere)
        aliases = {1: 0}
    return pl.pallas_call(
        functools.partial(scatter_kernel, tuple(moves)),
        out_shape=jax.ShapeDtypeStruct(out_shape, BF16),
        in_specs=in_specs,
        out_specs=anywhere,
        scratch_shapes=[pltpu.SemaphoreType.DMA((len(moves),))],
        input_output_aliases=aliases,
        compiler_params=limits(4),
        cost_estimate=cost(8e8),
    )(*operands)


def passed_round(value, axis):
    length = lax.axis_size(axis)
    return lax.ppermute(value, axis, [(i, (i + 1) % length) for i in range(length)])


def exchanged(value):
    return lax.all_to_all(value, "cp", split_axis=0, concat_axis=0, tiled=True)


def per_device(mixed_qkv, gate_z, gate_logits, block_table, conv_weight, a_log, dt_bias, norm_gain):
    cp_count = lax.axis_size("cp")
    seg_count = lax.axis_size("seg")
    cp_place = lax.axis_index("cp")
    rows = mixed_qkv.shape[0]
    heads = VALUE_HEADS // cp_count
    groups = max(1, heads // GROUP)
    share = heads // groups
    tiles = 1 + share
    key_width = KEY_HEADS * HEAD_DIM
    count = cp_count * rows // BLOCK
    gate_row = tiles * BLOCK

    order = jnp.argsort(block_table[0]).astype(jnp.int32)
    is_first = (lax.axis_index("seg") == 0).astype(jnp.int32).reshape(1)
    meta = jnp.concatenate([order, is_first])

    def key_head(place, group):
        return (place * heads + group * share) // GROUP

    def query_column(place, group):
        return key_head(place, group) * HEAD_DIM

    def inner_layout(group):
        rows_total = gate_row + 16
        tail_row = rows_total if group == groups - 1 else None
        return tail_row, rows_total + (16 * groups if group == groups - 1 else 0)

    def inner_moves(group):
        tail_row, _ = inner_layout(group)
        moves = []
        for place in range(cp_count):
            found = [key_width + key_head(place, group) * HEAD_DIM]
            for h in range(share):
                found.append(2 * key_width + (place * heads + group * share + h) * HEAD_DIM)
            for tile, column in enumerate(found):
                moves.append((0, 0, rows, column, place, tile * rows))
            if tail_row is not None:
                for other in range(groups):
                    column = query_column(place, other)
                    moves.append((0, rows - 16, 16, column, place, tail_row + 16 * other))
        return moves

    def outer_moves():
        moves = []
        for place in range(cp_count):
            for group in range(groups):
                moves.append((0, 0, rows, query_column(place, group), place, group * rows))
            for h in range(heads):
                column = (place * heads + h) * HEAD_DIM
                moves.append((1, 0, rows, column, place, (groups + h) * rows))
        return moves

    def halo(arrived, places):
        found = pl.pallas_call(
            functools.partial(halo_kernel, tuple(places)),
            out_shape=jax.ShapeDtypeStruct((len(places), 16, HEAD_DIM), BF16),
            in_specs=[smem, anywhere],
            out_specs=vmem,
            scratch_shapes=[pltpu.SemaphoreType.DMA((len(places),))],
            compiler_params=limits(2),
            cost_estimate=cost(1e8),
        )(meta, arrived)
        return passed_round(found, "seg")

    def in_hbm(array):
        return pltpu.with_memory_space_constraint(array, pltpu.HBM)

    received, tails = [], []
    for group in range(groups):
        tail_row, rows_total = inner_layout(group)
        sent = gather(
            [in_hbm(mixed_qkv)],
            inner_moves(group),
            cp_count,
            rows_total,
            logits=gate_logits.T,
            first_row=gate_row,
            heads=heads,
        )
        received.append(exchanged(sent))
        places = [tile * rows + rows - 16 for tile in range(tiles)]
        if tail_row is not None:
            places += [tail_row + 16 * other for other in range(groups)]
        tails.append(halo(received[group], places))

    packed = gather(
        [in_hbm(mixed_qkv), in_hbm(gate_z)], outer_moves(), cp_count, (groups + heads) * rows
    )
    outer = exchanged(packed)

    shaped = conv_weight.reshape(CONV, -1, HEAD_DIM)

    def taps(first, total):
        return lax.dynamic_slice_in_dim(shaped, first, total, 1).transpose(1, 0, 2)

    weights, query_weights = [], []
    for group in range(groups):
        own_key = key_head(cp_place, group)
        own_value = 2 * KEY_HEADS + cp_place * heads + group * share
        query_weights.append(taps(own_key, 1))
        weights.append(
            jnp.concatenate([taps(KEY_HEADS + own_key, 1), taps(own_value, share)], axis=0)
        )
    head_log = lax.dynamic_slice_in_dim(a_log, cp_place * heads, heads, 0)
    head_bias = lax.dynamic_slice_in_dim(dt_bias, cp_place * heads, heads, 0)
    rates = jnp.pad(jnp.stack([head_log, head_bias]), ((0, 0), (0, 8 - heads)))
    rates = jnp.broadcast_to(rates[:, :, None], (2, 8, BLOCK))

    def inner(group, first_block, blocks, last_part, earlier):
        per_step, per_chunk = min(4, blocks), min(8, blocks)
        dims = (group, share, first_block, blocks, per_step, per_chunk, last_part)
        wide = (share, count * BLOCK, 2 * HEAD_DIM)
        kept = (share, blocks * BLOCK, 2 * HEAD_DIM)
        out_shape = [
            pltpu.HBM(wide, F32),
            pltpu.HBM(wide, F32),
            pltpu.HBM((count, HEAD_DIM, BLOCK), F32),
            jax.ShapeDtypeStruct((2, blocks, 8, BLOCK), F32),
        ]
        if last_part:
            out_shape.append(jax.ShapeDtypeStruct((share, HEAD_DIM, HEAD_DIM), F32))
            out_shape.append(jax.ShapeDtypeStruct((share, HEAD_DIM, 2 * HEAD_DIM), BF16))
        else:
            out_shape.append(jax.ShapeDtypeStruct((share, HEAD_DIM, 2 * HEAD_DIM), F32))
        operands = [meta, received[group], tails[group], weights[group], rates]
        in_specs = [smem] + [vmem] * 4
        aliases = {}
        if earlier is not None:
            state, buffers = earlier
            operands += [state] + list(buffers)
            in_specs += [vmem] + [stored] * 3
            aliases = {6: 0, 7: 1, 8: 2}
        return pl.pallas_call(
            functools.partial(inner_kernel, dims),
            out_shape=out_shape,
            in_specs=in_specs,
            out_specs=[stored] * 3 + [vmem] * (len(out_shape) - 3),
            scratch_shapes=[
                pltpu.VMEM(kept, F32),
                pltpu.VMEM(kept, F32),
                pltpu.VMEM((blocks, HEAD_DIM, BLOCK), F32),
                pltpu.VMEM((per_chunk * tiles, 8 + BLOCK, HEAD_DIM), F32),
                pltpu.VMEM((len(LEVELS), BLOCK, BLOCK), BF16),
                pltpu.VMEM((share, HEAD_DIM, 2 * HEAD_DIM), F32),
                pltpu.SemaphoreType.DMA((3, blocks)),
            ],
            input_output_aliases=aliases,
            compiler_params=limits(INNER_MIB),
            cost_estimate=cost(6e8 * blocks * share),
        )(*operands)

    def chain(shift, over):
        incoming = None
        for rounds in range(seg_count - 1):
            advanced = shift
            if rounds:
                advanced = pl.pallas_call(
                    advance_kernel,
                    out_shape=jax.ShapeDtypeStruct(shift.shape, F32),
                    in_specs=[vmem] * 3,
                    out_specs=vmem,
                    compiler_params=limits(3),
                    cost_estimate=cost(2e8),
                )(shift, over, incoming)
            incoming = passed_round(advanced, "seg")
        if incoming is None:
            incoming = jnp.zeros_like(shift)
        return incoming

    def finish(group, counts, incoming, buffers, lines):
        gate_start = (groups + group * share) * rows
        dims = (group, share, tuple(counts), group * rows, gate_start, tiles + group)
        wide = (share, count * BLOCK, 2 * HEAD_DIM)
        operands = [meta, outer, tails[-1], query_weights[group], incoming]
        operands.append(norm_gain.reshape(1, HEAD_DIM))
        operands += [in_hbm(array) for array in buffers]
        operands += lines
        return pl.pallas_call(
            functools.partial(finish_kernel, dims),
            out_shape=jax.ShapeDtypeStruct((count, share * BLOCK, HEAD_DIM), BF16),
            in_specs=[smem] + [vmem] * 5 + [stored] * 3 + [vmem] * len(lines),
            out_specs=vmem,
            scratch_shapes=[
                pltpu.VMEM(wide, F32),
                pltpu.VMEM(wide, F32),
                pltpu.VMEM((count, HEAD_DIM, BLOCK), F32),
                pltpu.VMEM((4, 8 + BLOCK, HEAD_DIM), F32),
                pltpu.SemaphoreType.DMA((3, count)),
            ],
            compiler_params=limits(FINISH_MIB),
            cost_estimate=cost(1.5e9),
        )(*operands)

    result = None
    for group in range(groups):
        parts = 2 if group and count % 8 == 0 else 1
        blocks = count // parts
        earlier, lines = None, []
        for part in range(parts):
            *buffers, line, state, over = (
                *inner(group, part * blocks, blocks, part == parts - 1, earlier),
                *([None] if part < parts - 1 else []),
            )
            lines.append(line)
            earlier = (state, buffers)
        incoming = chain(state, over)
        done = finish(group, [blocks] * parts, incoming, buffers, lines)
        swapped = exchanged(done)
        moves = [
            (place, h * rows, rows, (place * heads + group * share + h) * HEAD_DIM)
            for place in range(cp_count)
            for h in range(share)
        ]
        result = scatter(swapped, moves, (rows, VALUE_HEADS * HEAD_DIM), result)
    return result


def solution(mesh):
    return jax.shard_map(
        per_device,
        mesh=mesh,
        in_specs=(
            P(("seg", "cp"), None),
            P(("seg", "cp"), None),
            P(("seg", "cp"), None),
            P("seg", None),
            P(),
            P(),
            P(),
            P(),
        ),
        out_specs=P(("seg", "cp"), None),
        check_vma=False,
    )
```

```python
import functools

import jax
import jax.numpy as jnp
from jax import lax
from jax.experimental import pallas as pl
from jax.experimental.pallas import tpu as pltpu
from jax.sharding import PartitionSpec as P


VALUE_HEADS = 32
KEY_HEADS = 16
HEAD_DIM = 128
CONV = 4
BLOCK = 128
GROUP = VALUE_HEADS // KEY_HEADS
LEVELS = (2, 4, 8, 16, 32, 64)

F32 = jnp.float32
BF16 = jnp.bfloat16


def dot(a, b):
    return jnp.dot(a, b, preferred_element_type=F32)


def split(x):
    high = x.astype(BF16)
    low = (x - high.astype(F32)).astype(BF16)
    return high, low


def beside(*parts):
    return jnp.concatenate(parts, axis=1)


def below(*parts):
    return jnp.concatenate(parts, axis=0)


def narrow_product(a, b):
    row = beside(b[0], b[1])
    both = dot(beside(a[0], a[1]), below(row, row))
    half = row.shape[1] // 2
    return both[:, :half] + both[:, half:]


def wide_product(a, b):
    return dot(beside(a[0], a[1]), below(b[0], b[0])) + dot(a[0], b[1])


def silu(v):
    return v / (1.0 + jnp.exp(-v))


def softplus(v):
    e = jnp.exp(-jnp.abs(v))
    s = e / (2.0 + e)
    t = s * s
    series = 1.0 / 19.0
    for odd in (17, 15, 13, 11, 9, 7, 5, 3, 1):
        series = series * t + 1.0 / odd
    return jnp.maximum(v, 0.0) + 2.0 * s * series


def together(*streams):
    alive = list(streams)
    while alive:
        for stream in list(alive):
            if next(stream, "over") == "over":
                alive.remove(stream)


def shifted_rows(meta_ref, recv_ref, rows_ref, slot, lead, n, first_row):
    piece_rows = BLOCK // 2
    place = meta_ref[jnp.maximum(2 * n - 1, 0)]
    start = first_row + (place % 2) * piece_rows + piece_rows - 16
    old = recv_ref[place // 2, pl.ds(pl.multiple_of(start, 16), 16), :].astype(F32)
    rows_ref[slot, 0:8, :] = jnp.where(n == 0, lead, old)[8:16]
    for half in range(2):
        place = meta_ref[2 * n + half]
        start = pl.multiple_of(first_row + (place % 2) * piece_rows, piece_rows)
        fresh = recv_ref[place // 2, pl.ds(start, piece_rows), :]
        begin = 8 + half * piece_rows
        rows_ref[slot, begin : begin + piece_rows, :] = fresh.astype(F32)


def convolved(rows_ref, slot, weight_ref, tile):
    summed = None
    for offset in range(CONV):
        begin = 8 - CONV + 1 + offset
        term = weight_ref[tile, offset : offset + 1, :] * rows_ref[slot, begin : begin + BLOCK, :]
        summed = term if summed is None else summed + term
    return silu(summed)


def unit_scale(matrix):
    return lax.rsqrt(jnp.sum(matrix * matrix, axis=-1, keepdims=True) + 1e-06)


def inner_kernel(dims, meta_ref, recv_ref, tail_ref, weight_ref, rate_ref, *refs):
    group, share, first_block, count, per_step, per_chunk, last_part = dims
    if first_block:
        given_ref = refs[0]
        refs = refs[4:]
    else:
        given_ref = None
    solved_out, state_out, flip_out, row_out, refs = *refs[:4], refs[4:]
    if last_part:
        shift_ref, map_ref, refs = *refs[:2], refs[2:]
    else:
        final_ref, refs = refs[0], refs[1:]
    solved_ref, before_ref, flip_ref, rows_ref, mask_ref, state_ref, sems = refs
    tiles = 1 + share
    gate_row = tiles * BLOCK
    piece_rows = BLOCK // 2
    is_first = meta_ref[meta_ref.shape[0] - 1]

    row_index = lax.broadcasted_iota(jnp.int32, (BLOCK, BLOCK), 0)
    col_index = lax.broadcasted_iota(jnp.int32, (BLOCK, BLOCK), 1)
    differ = row_index ^ col_index
    for place, size in enumerate(LEVELS):
        inside = (differ >= size) & (differ < 2 * size)
        mask_ref[place] = jnp.where(inside, 1.0, 0.0).astype(BF16)
    eye = jnp.where(row_index == col_index, 1.0, 0.0).astype(F32)
    strict = row_index > col_index
    upper = jnp.where(row_index <= col_index, 1.0, 0.0).astype(BF16)
    nothing = jnp.zeros((BLOCK, HEAD_DIM), F32)
    for h in range(share):
        state_ref[h] = beside(nothing, eye) if given_ref is None else given_ref[h]

    def leaving(kind, n):
        here = pl.ds(pl.multiple_of(n * BLOCK, BLOCK), BLOCK)
        there = pl.ds(pl.multiple_of((first_block + n) * BLOCK, BLOCK), BLOCK)
        source, target = ((solved_ref, solved_out), (before_ref, state_out))[kind]
        return pltpu.make_async_copy(source.at[:, here, :], target.at[:, there, :], sems.at[kind, n])

    def leaving_flip(n):
        return pltpu.make_async_copy(flip_ref.at[n], flip_out.at[first_block + n], sems.at[2, n])

    def chunk(number, carry):
        steps = []
        for step in range(per_chunk // per_step):
            blocks = [number * per_chunk + step * per_step + b for b in range(per_step)]
            steps.append(dict(blocks=blocks, slot=step * per_step * tiles))

        def prepare(work):
            blocks = work["blocks"]
            lane = lax.broadcasted_iota(jnp.int32, (16, BLOCK), 1)
            work["line"], work["beta"], work["end"], work["keys"], work["values"] = {}, {}, {}, {}, {}
            work["system"], work["inverse"], work["grow"] = {}, {}, {}
            for b, n in enumerate(blocks):
                picked = []
                for half in range(2):
                    place = meta_ref[2 * (first_block + n) + half]
                    found = recv_ref[place // 2, gate_row : gate_row + 16, :].astype(F32)
                    turned = pltpu.roll(found, piece_rows, 1)
                    picked.append(jnp.where(place % 2 == half, found, turned))
                logits = jnp.where(lane < piece_rows, picked[0], picked[1])
                beta = 1.0 / (1.0 + jnp.exp(-logits[0:8]))
                decay = -jnp.exp(rate_ref[0]) * softplus(logits[8:16] + rate_ref[1])
                high = decay.astype(BF16)
                remain = decay - high.astype(F32)
                middle = remain.astype(BF16)
                low = (remain - middle.astype(F32)).astype(BF16)
                stacked = below(high.astype(F32), middle.astype(F32), low.astype(F32))
                stacked = below(stacked, jnp.zeros((8, BLOCK), F32)).astype(BF16)
                sums = dot(stacked, upper)
                cum = sums[0:8] + sums[8:16] + sums[16:24]
                row_out[0, n] = cum
                row_out[1, n] = beta
                work["line"][b], work["beta"][b] = cum, beta
                work["end"][b] = jnp.broadcast_to(cum[:, BLOCK - 1 :], (8, BLOCK))
                yield
            for b, n in enumerate(blocks):
                for tile in range(tiles):
                    slot = work["slot"] + b * tiles + tile
                    lead = jnp.where(is_first == 1, 0.0, tail_ref[tile].astype(F32))
                    shifted_rows(meta_ref, recv_ref, rows_ref, slot, lead, first_block + n, tile * BLOCK)
                    active = convolved(rows_ref, slot, weight_ref, tile)
                    if tile == 0:
                        work["keys"][b] = active * unit_scale(active)
                    else:
                        work["values"][b, tile - 1] = active
                    yield
                turned = work["keys"][b].T
                flip_ref[n] = turned
                leaving_flip(n).start()
                gram = narrow_product(split(work["keys"][b]), split(turned))
                yield
                columns = below(work["line"][b], jnp.zeros((BLOCK - 8, BLOCK), F32)).T
                for h in range(share):
                    at = group * share + h
                    column = jnp.broadcast_to(columns[:, at : at + 1], (BLOCK, BLOCK))
                    decay = jnp.exp(jnp.where(strict, column - work["line"][b][at : at + 1], 0.0))
                    work["grow"][b, h] = jnp.exp(column)
                    scaled = decay * work["beta"][b][at : at + 1]
                    lower = jnp.where(strict, gram * scaled, 0.0)
                    work["system"][b, h] = split(lower)
                    work["inverse"][b, h] = eye - jnp.where(differ == 1, lower, 0.0)
                    yield

        def invert(work):
            inverse, system = work["inverse"], work["system"]
            for place, size in enumerate(LEVELS):
                mask = mask_ref[place]
                halves, cross = {}, {}
                for u in inverse:
                    halves[u] = split(inverse[u])
                    parts = (system[u][0] * mask, system[u][1] * mask)
                    cross[u] = split(narrow_product(parts, halves[u]))
                    yield
                for u in inverse:
                    inverse[u] = inverse[u] - narrow_product(halves[u], cross[u])
                    yield

        def advance(work):
            blocks = work["blocks"]
            solved, shift, over, keep = {}, {}, {}, {}
            for b, n in enumerate(blocks):
                at = pl.ds(pl.multiple_of(n * BLOCK, BLOCK), BLOCK)
                for h in range(share):
                    row = group * share + h
                    right = split(beside(work["values"][b, h], work["keys"][b] * work["grow"][b, h]))
                    found = wide_product(split(work["inverse"][b, h]), right)
                    solved_ref[h, at, :] = found
                    solved[b, h] = split(found)
                    yield
                leaving(0, n).start()
            for b, n in enumerate(blocks):
                for h in range(share):
                    row = group * share + h
                    end, line = work["end"][b][row : row + 1], work["line"][b][row : row + 1]
                    weight = jnp.exp(end - line) * work["beta"][b][row : row + 1]
                    moved = wide_product(split(flip_ref[n] * weight), solved[b, h])
                    shift[b, h] = moved[:, :HEAD_DIM]
                    over[b, h] = split(moved[:, HEAD_DIM:])
                    keep[b, h] = beside(jnp.exp(end), jnp.exp(end))
                    yield
            for b, n in enumerate(blocks):
                at = pl.ds(pl.multiple_of(n * BLOCK, BLOCK), BLOCK)
                for h in range(share):
                    state = state_ref[h]
                    before_ref[h, at, :] = state
                    moved = wide_product(over[b, h], split(state))
                    state_ref[h] = state * keep[b, h] + beside(shift[b, h], nothing) - moved
                    yield
                leaving(1, n).start()

        together(prepare(steps[0]))
        for place, work in enumerate(steps):
            streams = [invert(work)]
            if place + 1 < len(steps):
                streams.append(prepare(steps[place + 1]))
            if place:
                streams.append(advance(steps[place - 1]))
            together(*streams)
        together(advance(steps[-1]))
        return carry

    if count == per_chunk:
        chunk(0, 0)
    else:
        lax.fori_loop(0, count // per_chunk, chunk, 0)
    for h in range(share):
        if last_part:
            shift_ref[h] = state_ref[h, :, :HEAD_DIM]
            over = jnp.where(is_first == 1, 0.0, state_ref[h, :, HEAD_DIM:])
            map_high, map_low = split(over)
            map_ref[h] = beside(map_high, map_low)
        else:
            final_ref[h] = state_ref[h]

    def drain(n, carry):
        leaving(0, n).wait()
        leaving(1, n).wait()
        leaving_flip(n).wait()
        return carry

    lax.fori_loop(0, count, drain, 0)


def advance_kernel(shift_ref, map_ref, incoming_ref, out_ref):
    for h in range(shift_ref.shape[0]):
        high, low = split(incoming_ref[h])
        row = beside(high, low)
        both = dot(map_ref[h], below(row, row))
        out_ref[h] = shift_ref[h] + both[:, :HEAD_DIM] + both[:, HEAD_DIM:]


def finish_kernel(
    dims,
    meta_ref,
    outer_ref,
    tail_ref,
    weight_ref,
    incoming_ref,
    gain_ref,
    solved_in,
    state_in,
    flip_in,
    *refs,
):
    group, share, counts, query_row, gate_row, tail_place = dims
    count = sum(counts)
    line_refs = refs[: len(counts)]
    out_ref, solved_ref, before_ref, flip_ref, rows_ref, sems = refs[len(counts) :]
    piece_rows = BLOCK // 2
    is_first = meta_ref[meta_ref.shape[0] - 1]
    row_index = lax.broadcasted_iota(jnp.int32, (BLOCK, BLOCK), 0)
    col_index = lax.broadcasted_iota(jnp.int32, (BLOCK, BLOCK), 1)
    inclusive = row_index >= col_index

    def arriving(n):
        at = pl.ds(pl.multiple_of(n * BLOCK, BLOCK), BLOCK)
        return (
            pltpu.make_async_copy(flip_in.at[n], flip_ref.at[n], sems.at[0, n]),
            pltpu.make_async_copy(state_in.at[:, at, :], before_ref.at[:, at, :], sems.at[1, n]),
            pltpu.make_async_copy(solved_in.at[:, at, :], solved_ref.at[:, at, :], sems.at[2, n]),
        )

    def fetch(n, carry):
        for copy in arriving(n):
            copy.start()
        return carry

    lax.fori_loop(0, count, fetch, 0)
    entry = [split(jnp.where(is_first == 1, 0.0, incoming_ref[h])) for h in range(share)]

    def step(index, carry, first_block, per_step, row_ref):
        spots = [index * per_step + b for b in range(per_step)]
        blocks = [first_block + spot for spot in spots]
        queries, grams = {}, {}
        for b, n in enumerate(blocks):
            lead = jnp.where(is_first == 1, 0.0, tail_ref[tail_place].astype(F32))
            shifted_rows(meta_ref, outer_ref, rows_ref, b, lead, n, query_row)
            active = convolved(rows_ref, b, weight_ref, 0)
            queries[b] = active * (unit_scale(active) * HEAD_DIM ** (-0.5))
        for n in blocks:
            for copy in arriving(n):
                copy.wait()
        for b, n in enumerate(blocks):
            grams[b] = narrow_product(split(queries[b]), split(flip_ref[n]))
        units = [(b, h) for b in range(per_step) for h in range(share)]
        lefts, states, fresh = {}, {}, {}
        for b, h in units:
            n = blocks[b]
            at = group * share + h
            cum, beta = row_ref[0, spots[b]], row_ref[1, spots[b]]
            columns = below(cum, jnp.zeros((BLOCK - 8, BLOCK), F32)).T
            column = jnp.broadcast_to(columns[:, at : at + 1], (BLOCK, BLOCK))
            decay = jnp.exp(jnp.where(inclusive, column - cum[at : at + 1], 0.0))
            attend = jnp.where(inclusive, grams[b] * decay * beta[at : at + 1], 0.0)
            q_high, q_low = split(queries[b] * jnp.exp(column))
            a_high, a_low = split(attend)
            lefts[b, h] = (beside(q_high, a_high), beside(q_low, a_low))
        for b, h in units:
            rows = pl.ds(pl.multiple_of(blocks[b] * BLOCK, BLOCK), BLOCK)
            shift = before_ref[h, rows, :HEAD_DIM]
            over = split(before_ref[h, rows, HEAD_DIM:])
            states[b, h] = split(shift + narrow_product(over, entry[h]))
        for b, h in units:
            rows = pl.ds(pl.multiple_of(blocks[b] * BLOCK, BLOCK), BLOCK)
            px = split(solved_ref[h, rows, HEAD_DIM:])
            ux = solved_ref[h, rows, :HEAD_DIM]
            fresh[b, h] = split(ux - narrow_product(px, states[b, h]))
        for b, h in units:
            n = blocks[b]
            right = below(beside(*states[b, h]), beside(*fresh[b, h]))
            both = dot(lefts[b, h][0], right) + dot(lefts[b, h][1], right)
            core = both[:, :HEAD_DIM] + both[:, HEAD_DIM:]
            scale = lax.rsqrt(jnp.mean(core * core, axis=-1, keepdims=True) + 1e-06)
            gates = []
            for half in range(2):
                place = meta_ref[2 * n + half]
                start = gate_row + h * BLOCK + (place % 2) * piece_rows
                start = pl.multiple_of(start, piece_rows)
                gates.append(outer_ref[place // 2, pl.ds(start, piece_rows), :].astype(F32))
            gate = below(*gates)
            result = core * scale * gain_ref[...] * silu(gate)
            out_ref[n, h * BLOCK : (h + 1) * BLOCK, :] = result.astype(BF16)
        return carry

    first_block = 0
    for blocks, row_ref in zip(counts, line_refs):
        per_step = min(4, blocks)
        part = functools.partial(step, first_block=first_block, per_step=per_step, row_ref=row_ref)
        if blocks == per_step:
            part(0, 0)
        else:
            lax.fori_loop(0, blocks // per_step, part, 0)
        first_block += blocks


def gather_kernel(moves, source_count, logit_place, *refs):
    sources, refs = refs[:source_count], refs[source_count:]
    if logit_place:
        logit_ref, out_ref, sems, wide_ref, plain_ref, logit_sem = refs
        fetch = pltpu.make_async_copy(logit_ref, plain_ref, logit_sem.at[0])
        fetch.start()
    else:
        out_ref, sems = refs
    copies = []
    for number, (source, begin, length, column, place, row) in enumerate(moves):
        copies.append(
            pltpu.make_async_copy(
                sources[source].at[pl.ds(begin, length), pl.ds(column, HEAD_DIM)],
                out_ref.at[place, pl.ds(row, length), :],
                sems.at[number],
            )
        )
    for copy in copies:
        copy.start()
    if logit_place:
        first_row, heads = logit_place
        wide_ref[...] = jnp.zeros(wide_ref.shape, F32)
        fetch.wait()
        wide_ref[0 : 2 * VALUE_HEADS, :] = plain_ref[...].astype(F32)
        for place in range(out_ref.shape[0]):
            begin = place * heads
            rates = wide_ref[begin : begin + 8, :]
            steps = wide_ref[VALUE_HEADS + begin : VALUE_HEADS + begin + 8, :]
            out_ref[place, first_row : first_row + 16, :] = below(rates, steps).astype(BF16)
    for copy in copies:
        copy.wait()


def halo_kernel(places, meta_ref, arrived_ref, out_ref, sems):
    last = meta_ref[meta_ref.shape[0] - 2]
    copies = []
    for tile, row in enumerate(places):
        source = arrived_ref.at[last // 2, pl.ds(row, 16), :]
        copies.append(pltpu.make_async_copy(source, out_ref.at[tile], sems.at[tile]))
    for copy in copies:
        copy.start()
    for copy in copies:
        copy.wait()


def scatter_kernel(moves, *refs):
    source_ref, out_ref, sems = refs[0], refs[-2], refs[-1]
    copies = []
    for number, (place, row, length, column) in enumerate(moves):
        copies.append(
            pltpu.make_async_copy(
                source_ref.at[place, pl.ds(row, length), :],
                out_ref.at[:, pl.ds(column, HEAD_DIM)],
                sems.at[number],
            )
        )
    for copy in copies:
        copy.start()
    for copy in copies:
        copy.wait()


MIB = 2**20
GATHER_MIB = 6
INNER_MIB = 24
FINISH_MIB = 20


def limits(mib):
    return pltpu.CompilerParams(vmem_limit_bytes=mib * MIB)


def cost(flops):
    return pl.CostEstimate(flops=int(flops), bytes_accessed=2**20, transcendentals=0)


vmem = pl.BlockSpec(memory_space=pltpu.VMEM)
smem = pl.BlockSpec(memory_space=pltpu.SMEM)
anywhere = pl.BlockSpec(memory_space=pl.ANY)
stored = pl.BlockSpec(memory_space=pltpu.HBM)


def gather(sources, moves, places, rows, logits=None, first_row=0, heads=0):
    operands, in_specs = list(sources), [anywhere] * len(sources)
    scratch = [pltpu.SemaphoreType.DMA((len(moves),))]
    logit_place = None
    if logits is not None:
        operands.append(logits)
        in_specs.append(anywhere)
        scratch.append(pltpu.VMEM((2 * VALUE_HEADS + 8, logits.shape[1]), F32))
        scratch.append(pltpu.VMEM(logits.shape, BF16))
        scratch.append(pltpu.SemaphoreType.DMA((1,)))
        logit_place = (first_row, heads)
    return pl.pallas_call(
        functools.partial(gather_kernel, tuple(moves), len(sources), logit_place),
        out_shape=jax.ShapeDtypeStruct((places, rows, HEAD_DIM), BF16),
        in_specs=in_specs,
        out_specs=vmem,
        scratch_shapes=scratch,
        compiler_params=limits(GATHER_MIB),
        cost_estimate=cost(8e8),
    )(*operands)


def scatter(source, moves, out_shape, base=None):
    operands, in_specs, aliases = [source], [vmem], {}
    if base is not None:
        operands.append(base)
        in_specs.append(anywhere)
        aliases = {1: 0}
    return pl.pallas_call(
        functools.partial(scatter_kernel, tuple(moves)),
        out_shape=jax.ShapeDtypeStruct(out_shape, BF16),
        in_specs=in_specs,
        out_specs=anywhere,
        scratch_shapes=[pltpu.SemaphoreType.DMA((len(moves),))],
        input_output_aliases=aliases,
        compiler_params=limits(4),
        cost_estimate=cost(8e8),
    )(*operands)


def passed_round(value, axis):
    length = lax.axis_size(axis)
    return lax.ppermute(value, axis, [(i, (i + 1) % length) for i in range(length)])


def exchanged(value):
    return lax.all_to_all(value, "cp", split_axis=0, concat_axis=0, tiled=True)


def per_device(mixed_qkv, gate_z, gate_logits, block_table, conv_weight, a_log, dt_bias, norm_gain):
    cp_count = lax.axis_size("cp")
    seg_count = lax.axis_size("seg")
    cp_place = lax.axis_index("cp")
    rows = mixed_qkv.shape[0]
    heads = VALUE_HEADS // cp_count
    groups = max(1, heads // GROUP)
    share = heads // groups
    tiles = 1 + share
    key_width = KEY_HEADS * HEAD_DIM
    count = cp_count * rows // BLOCK
    gate_row = tiles * BLOCK

    order = jnp.argsort(block_table[0]).astype(jnp.int32)
    is_first = (lax.axis_index("seg") == 0).astype(jnp.int32).reshape(1)
    meta = jnp.concatenate([order, is_first])

    def key_head(place, group):
        return (place * heads + group * share) // GROUP

    def query_column(place, group):
        return key_head(place, group) * HEAD_DIM

    def inner_layout(group):
        later = [other for other in range(1, groups)] if group == 0 else []
        asked = groups if group == groups - 1 else 0
        tail_row = gate_row + 16
        return later, asked, tail_row, tail_row + 16 * (len(later) * tiles + asked)

    def inner_columns(place, group):
        found = [key_width + key_head(place, group) * HEAD_DIM]
        for h in range(share):
            found.append(2 * key_width + (place * heads + group * share + h) * HEAD_DIM)
        return found

    def inner_moves(group):
        later, asked, tail_row, _ = inner_layout(group)
        moves = []
        for place in range(cp_count):
            for tile, column in enumerate(inner_columns(place, group)):
                moves.append((0, 0, rows, column, place, tile * rows))
            extra = [column for other in later for column in inner_columns(place, other)]
            extra += [query_column(place, other) for other in range(asked)]
            for spot, column in enumerate(extra):
                moves.append((0, rows - 16, 16, column, place, tail_row + 16 * spot))
        return moves

    def outer_moves():
        moves = []
        for place in range(cp_count):
            for group in range(groups):
                moves.append((0, 0, rows, query_column(place, group), place, group * rows))
            for h in range(heads):
                column = (place * heads + h) * HEAD_DIM
                moves.append((1, 0, rows, column, place, (groups + h) * rows))
        return moves

    def halo(arrived, places):
        found = pl.pallas_call(
            functools.partial(halo_kernel, tuple(places)),
            out_shape=jax.ShapeDtypeStruct((len(places), 16, HEAD_DIM), BF16),
            in_specs=[smem, anywhere],
            out_specs=vmem,
            scratch_shapes=[pltpu.SemaphoreType.DMA((len(places),))],
            compiler_params=limits(2),
            cost_estimate=cost(1e8),
        )(meta, arrived)
        return passed_round(found, "seg")

    def in_hbm(array):
        return pltpu.with_memory_space_constraint(array, pltpu.HBM)

    received = []
    for group in range(groups):
        later, asked, tail_row, rows_total = inner_layout(group)
        sent = gather(
            [in_hbm(mixed_qkv)],
            inner_moves(group),
            cp_count,
            rows_total,
            logits=in_hbm(gate_logits.T),
            first_row=gate_row,
            heads=heads,
        )
        received.append(exchanged(sent))
        places = [tile * rows + rows - 16 for tile in range(tiles)] if group == 0 else []
        places += [tail_row + 16 * spot for spot in range(len(later) * tiles + asked)]
        if places:
            arrived = halo(received[group], places)
            if group == 0:
                tails = [arrived[other * tiles : (other + 1) * tiles] for other in range(groups)]
            query_tails = arrived[len(places) - asked :]

    packed = gather(
        [in_hbm(mixed_qkv), in_hbm(gate_z)], outer_moves(), cp_count, (groups + heads) * rows
    )
    outer = exchanged(packed)

    shaped = conv_weight.reshape(CONV, -1, HEAD_DIM)

    def taps(first, total):
        return lax.dynamic_slice_in_dim(shaped, first, total, 1).transpose(1, 0, 2)

    weights, query_weights = [], []
    for group in range(groups):
        own_key = key_head(cp_place, group)
        own_value = 2 * KEY_HEADS + cp_place * heads + group * share
        query_weights.append(taps(own_key, 1))
        weights.append(
            jnp.concatenate([taps(KEY_HEADS + own_key, 1), taps(own_value, share)], axis=0)
        )
    head_log = lax.dynamic_slice_in_dim(a_log, cp_place * heads, heads, 0)
    head_bias = lax.dynamic_slice_in_dim(dt_bias, cp_place * heads, heads, 0)
    rates = jnp.pad(jnp.stack([head_log, head_bias]), ((0, 0), (0, 8 - heads)))
    rates = jnp.broadcast_to(rates[:, :, None], (2, 8, BLOCK))

    def inner(group, first_block, blocks, last_part, earlier):
        per_step, per_chunk = min(4, blocks), min(8, blocks)
        dims = (group, share, first_block, blocks, per_step, per_chunk, last_part)
        wide = (share, count * BLOCK, 2 * HEAD_DIM)
        kept = (share, blocks * BLOCK, 2 * HEAD_DIM)
        out_shape = [
            pltpu.HBM(wide, F32),
            pltpu.HBM(wide, F32),
            pltpu.HBM((count, HEAD_DIM, BLOCK), F32),
            jax.ShapeDtypeStruct((2, blocks, 8, BLOCK), F32),
        ]
        if last_part:
            out_shape.append(jax.ShapeDtypeStruct((share, HEAD_DIM, HEAD_DIM), F32))
            out_shape.append(jax.ShapeDtypeStruct((share, HEAD_DIM, 2 * HEAD_DIM), BF16))
        else:
            out_shape.append(jax.ShapeDtypeStruct((share, HEAD_DIM, 2 * HEAD_DIM), F32))
        operands = [meta, received[group], tails[group], weights[group], rates]
        in_specs = [smem] + [vmem] * 4
        aliases = {}
        if earlier is not None:
            state, buffers = earlier
            operands += [state] + list(buffers)
            in_specs += [vmem] + [stored] * 3
            aliases = {6: 0, 7: 1, 8: 2}
        return pl.pallas_call(
            functools.partial(inner_kernel, dims),
            out_shape=out_shape,
            in_specs=in_specs,
            out_specs=[stored] * 3 + [vmem] * (len(out_shape) - 3),
            scratch_shapes=[
                pltpu.VMEM(kept, F32),
                pltpu.VMEM(kept, F32),
                pltpu.VMEM((blocks, HEAD_DIM, BLOCK), F32),
                pltpu.VMEM((per_chunk * tiles, 8 + BLOCK, HEAD_DIM), F32),
                pltpu.VMEM((len(LEVELS), BLOCK, BLOCK), BF16),
                pltpu.VMEM((share, HEAD_DIM, 2 * HEAD_DIM), F32),
                pltpu.SemaphoreType.DMA((3, blocks)),
            ],
            input_output_aliases=aliases,
            compiler_params=limits(INNER_MIB),
            cost_estimate=cost(6e8 * blocks * share),
        )(*operands)

    def chain(shift, over):
        incoming = None
        for rounds in range(seg_count - 1):
            advanced = shift
            if rounds:
                advanced = pl.pallas_call(
                    advance_kernel,
                    out_shape=jax.ShapeDtypeStruct(shift.shape, F32),
                    in_specs=[vmem] * 3,
                    out_specs=vmem,
                    compiler_params=limits(3),
                    cost_estimate=cost(2e8),
                )(shift, over, incoming)
            incoming = passed_round(advanced, "seg")
        if incoming is None:
            incoming = jnp.zeros_like(shift)
        return incoming

    def finish(group, counts, incoming, buffers, lines):
        gate_start = (groups + group * share) * rows
        dims = (group, share, tuple(counts), group * rows, gate_start, group)
        wide = (share, count * BLOCK, 2 * HEAD_DIM)
        operands = [meta, outer, query_tails, query_weights[group], incoming]
        operands.append(norm_gain.reshape(1, HEAD_DIM))
        operands += [in_hbm(array) for array in buffers]
        operands += lines
        return pl.pallas_call(
            functools.partial(finish_kernel, dims),
            out_shape=jax.ShapeDtypeStruct((count, share * BLOCK, HEAD_DIM), BF16),
            in_specs=[smem] + [vmem] * 5 + [stored] * 3 + [vmem] * len(lines),
            out_specs=vmem,
            scratch_shapes=[
                pltpu.VMEM(wide, F32),
                pltpu.VMEM(wide, F32),
                pltpu.VMEM((count, HEAD_DIM, BLOCK), F32),
                pltpu.VMEM((4, 8 + BLOCK, HEAD_DIM), F32),
                pltpu.SemaphoreType.DMA((3, count)),
            ],
            compiler_params=limits(FINISH_MIB),
            cost_estimate=cost(1.5e9),
        )(*operands)

    result = None
    for group in range(groups):
        parts = 2 if group and count % 8 == 0 else 1
        blocks = count // parts
        earlier, lines = None, []
        for part in range(parts):
            *buffers, line, state, over = (
                *inner(group, part * blocks, blocks, part == parts - 1, earlier),
                *([None] if part < parts - 1 else []),
            )
            lines.append(line)
            earlier = (state, buffers)
        incoming = chain(state, over)
        done = finish(group, [blocks] * parts, incoming, buffers, lines)
        swapped = exchanged(done)
        moves = [
            (place, h * rows, rows, (place * heads + group * share + h) * HEAD_DIM)
            for place in range(cp_count)
            for h in range(share)
        ]
        result = scatter(swapped, moves, (rows, VALUE_HEADS * HEAD_DIM), result)
    return result


def solution(mesh):
    return jax.shard_map(
        per_device,
        mesh=mesh,
        in_specs=(
            P(("seg", "cp"), None),
            P(("seg", "cp"), None),
            P(("seg", "cp"), None),
            P("seg", None),
            P(),
            P(),
            P(),
            P(),
        ),
        out_specs=P(("seg", "cp"), None),
        check_vma=False,
    )
```

```python
import functools

import jax
import jax.numpy as jnp
from jax import lax
from jax.experimental import pallas as pl
from jax.experimental.pallas import tpu as pltpu
from jax.sharding import PartitionSpec as P


VALUE_HEADS = 32
KEY_HEADS = 16
HEAD_DIM = 128
CONV = 4
BLOCK = 128
GROUP = VALUE_HEADS // KEY_HEADS
LEVELS = (2, 4, 8, 16, 32, 64)

F32 = jnp.float32
BF16 = jnp.bfloat16


def dot(a, b):
    return jnp.dot(a, b, preferred_element_type=F32)


def split(x):
    high = x.astype(BF16)
    low = (x - high.astype(F32)).astype(BF16)
    return high, low


def beside(*parts):
    return jnp.concatenate(parts, axis=1)


def below(*parts):
    return jnp.concatenate(parts, axis=0)


def narrow_product(a, b):
    row = beside(b[0], b[1])
    both = dot(beside(a[0], a[1]), below(row, row))
    half = row.shape[1] // 2
    return both[:, :half] + both[:, half:]


def wide_product(a, b):
    return dot(beside(a[0], a[1]), below(b[0], b[0])) + dot(a[0], b[1])


def silu(v):
    return v / (1.0 + jnp.exp(-v))


def softplus(v):
    e = jnp.exp(-jnp.abs(v))
    s = e / (2.0 + e)
    t = s * s
    series = 1.0 / 19.0
    for odd in (17, 15, 13, 11, 9, 7, 5, 3, 1):
        series = series * t + 1.0 / odd
    return jnp.maximum(v, 0.0) + 2.0 * s * series


def together(*streams):
    alive = list(streams)
    while alive:
        for stream in list(alive):
            if next(stream, "over") == "over":
                alive.remove(stream)


def shifted_rows(meta_ref, recv_ref, rows_ref, slot, lead, n, first_row):
    piece_rows = BLOCK // 2
    place = meta_ref[jnp.maximum(2 * n - 1, 0)]
    start = first_row + (place % 2) * piece_rows + piece_rows - 16
    old = recv_ref[place // 2, pl.ds(pl.multiple_of(start, 16), 16), :].astype(F32)
    rows_ref[slot, 0:8, :] = jnp.where(n == 0, lead, old)[8:16]
    for half in range(2):
        place = meta_ref[2 * n + half]
        start = pl.multiple_of(first_row + (place % 2) * piece_rows, piece_rows)
        fresh = recv_ref[place // 2, pl.ds(start, piece_rows), :]
        begin = 8 + half * piece_rows
        rows_ref[slot, begin : begin + piece_rows, :] = fresh.astype(F32)


def convolved(rows_ref, slot, weight_ref, tile):
    summed = None
    for offset in range(CONV):
        begin = 8 - CONV + 1 + offset
        term = weight_ref[tile, offset : offset + 1, :] * rows_ref[slot, begin : begin + BLOCK, :]
        summed = term if summed is None else summed + term
    return silu(summed)


def unit_scale(matrix):
    return lax.rsqrt(jnp.sum(matrix * matrix, axis=-1, keepdims=True) + 1e-06)


def inner_kernel(dims, meta_ref, recv_ref, tail_ref, weight_ref, rate_ref, *refs):
    group, share, first_block, count, per_step, per_chunk, last_part = dims
    if first_block:
        given_ref = refs[0]
        refs = refs[4:]
    else:
        given_ref = None
    solved_out, state_out, flip_out, row_out, refs = *refs[:4], refs[4:]
    if last_part:
        shift_ref, map_ref, refs = *refs[:2], refs[2:]
    else:
        final_ref, refs = refs[0], refs[1:]
    solved_ref, before_ref, flip_ref, rows_ref, mask_ref, state_ref, sems = refs
    tiles = 1 + share
    gate_row = tiles * BLOCK
    piece_rows = BLOCK // 2
    is_first = meta_ref[meta_ref.shape[0] - 1]

    row_index = lax.broadcasted_iota(jnp.int32, (BLOCK, BLOCK), 0)
    col_index = lax.broadcasted_iota(jnp.int32, (BLOCK, BLOCK), 1)
    differ = row_index ^ col_index
    for place, size in enumerate(LEVELS):
        inside = (differ >= size) & (differ < 2 * size)
        mask_ref[place] = jnp.where(inside, 1.0, 0.0).astype(BF16)
    eye = jnp.where(row_index == col_index, 1.0, 0.0).astype(F32)
    strict = row_index > col_index
    upper = jnp.where(row_index <= col_index, 1.0, 0.0).astype(BF16)
    nothing = jnp.zeros((BLOCK, HEAD_DIM), F32)
    for h in range(share):
        state_ref[h] = beside(nothing, eye) if given_ref is None else given_ref[h]

    def leaving(kind, n):
        here = pl.ds(pl.multiple_of(n * BLOCK, BLOCK), BLOCK)
        there = pl.ds(pl.multiple_of((first_block + n) * BLOCK, BLOCK), BLOCK)
        source, target = ((solved_ref, solved_out), (before_ref, state_out))[kind]
        return pltpu.make_async_copy(source.at[:, here, :], target.at[:, there, :], sems.at[kind, n])

    def leaving_flip(n):
        return pltpu.make_async_copy(flip_ref.at[n], flip_out.at[first_block + n], sems.at[2, n])

    def chunk(number, carry):
        steps = []
        for step in range(per_chunk // per_step):
            blocks = [number * per_chunk + step * per_step + b for b in range(per_step)]
            steps.append(dict(blocks=blocks, slot=step * per_step * tiles))

        def prepare(work):
            blocks = work["blocks"]
            lane = lax.broadcasted_iota(jnp.int32, (16, BLOCK), 1)
            work["line"], work["beta"], work["end"], work["keys"], work["values"] = {}, {}, {}, {}, {}
            work["system"], work["inverse"], work["grow"] = {}, {}, {}
            for b, n in enumerate(blocks):
                picked = []
                for half in range(2):
                    place = meta_ref[2 * (first_block + n) + half]
                    found = recv_ref[place // 2, gate_row : gate_row + 16, :].astype(F32)
                    turned = pltpu.roll(found, piece_rows, 1)
                    picked.append(jnp.where(place % 2 == half, found, turned))
                logits = jnp.where(lane < piece_rows, picked[0], picked[1])
                beta = 1.0 / (1.0 + jnp.exp(-logits[0:8]))
                decay = -jnp.exp(rate_ref[0]) * softplus(logits[8:16] + rate_ref[1])
                high = decay.astype(BF16)
                remain = decay - high.astype(F32)
                middle = remain.astype(BF16)
                low = (remain - middle.astype(F32)).astype(BF16)
                stacked = below(high.astype(F32), middle.astype(F32), low.astype(F32))
                stacked = below(stacked, jnp.zeros((8, BLOCK), F32)).astype(BF16)
                sums = dot(stacked, upper)
                cum = sums[0:8] + sums[8:16] + sums[16:24]
                row_out[0, n] = cum
                row_out[1, n] = beta
                work["line"][b], work["beta"][b] = cum, beta
                work["end"][b] = jnp.broadcast_to(cum[:, BLOCK - 1 :], (8, BLOCK))
                yield
            for b, n in enumerate(blocks):
                for tile in range(tiles):
                    slot = work["slot"] + b * tiles + tile
                    lead = jnp.where(is_first == 1, 0.0, tail_ref[tile].astype(F32))
                    shifted_rows(meta_ref, recv_ref, rows_ref, slot, lead, first_block + n, tile * BLOCK)
                    active = convolved(rows_ref, slot, weight_ref, tile)
                    if tile == 0:
                        work["keys"][b] = active * unit_scale(active)
                    else:
                        work["values"][b, tile - 1] = active
                    yield
                turned = work["keys"][b].T
                flip_ref[n] = turned
                leaving_flip(n).start()
                gram = narrow_product(split(work["keys"][b]), split(turned))
                yield
                columns = below(work["line"][b], jnp.zeros((BLOCK - 8, BLOCK), F32)).T
                for h in range(share):
                    at = group * share + h
                    column = jnp.broadcast_to(columns[:, at : at + 1], (BLOCK, BLOCK))
                    decay = jnp.exp(jnp.where(strict, column - work["line"][b][at : at + 1], 0.0))
                    work["grow"][b, h] = jnp.exp(column)
                    scaled = decay * work["beta"][b][at : at + 1]
                    lower = jnp.where(strict, gram * scaled, 0.0)
                    work["system"][b, h] = split(lower)
                    work["inverse"][b, h] = eye - jnp.where(differ == 1, lower, 0.0)
                    yield

        def invert(work):
            inverse, system = work["inverse"], work["system"]
            for place, size in enumerate(LEVELS):
                mask = mask_ref[place]
                halves, cross = {}, {}
                for u in inverse:
                    halves[u] = split(inverse[u])
                    parts = (system[u][0] * mask, system[u][1] * mask)
                    cross[u] = split(narrow_product(parts, halves[u]))
                    yield
                for u in inverse:
                    inverse[u] = inverse[u] - narrow_product(halves[u], cross[u])
                    yield

        def advance(work):
            blocks = work["blocks"]
            solved, shift, over, keep = {}, {}, {}, {}
            for b, n in enumerate(blocks):
                at = pl.ds(pl.multiple_of(n * BLOCK, BLOCK), BLOCK)
                for h in range(share):
                    row = group * share + h
                    right = split(beside(work["values"][b, h], work["keys"][b] * work["grow"][b, h]))
                    found = wide_product(split(work["inverse"][b, h]), right)
                    solved_ref[h, at, :] = found
                    solved[b, h] = split(found)
                    yield
                leaving(0, n).start()
            for b, n in enumerate(blocks):
                for h in range(share):
                    row = group * share + h
                    end, line = work["end"][b][row : row + 1], work["line"][b][row : row + 1]
                    weight = jnp.exp(end - line) * work["beta"][b][row : row + 1]
                    moved = wide_product(split(flip_ref[n] * weight), solved[b, h])
                    shift[b, h] = moved[:, :HEAD_DIM]
                    over[b, h] = split(moved[:, HEAD_DIM:])
                    keep[b, h] = beside(jnp.exp(end), jnp.exp(end))
                    yield
            for b, n in enumerate(blocks):
                at = pl.ds(pl.multiple_of(n * BLOCK, BLOCK), BLOCK)
                for h in range(share):
                    state = state_ref[h]
                    before_ref[h, at, :] = state
                    moved = wide_product(over[b, h], split(state))
                    state_ref[h] = state * keep[b, h] + beside(shift[b, h], nothing) - moved
                    yield
                leaving(1, n).start()

        together(prepare(steps[0]))
        for place, work in enumerate(steps):
            streams = [invert(work)]
            if place + 1 < len(steps):
                streams.append(prepare(steps[place + 1]))
            if place:
                streams.append(advance(steps[place - 1]))
            together(*streams)
        together(advance(steps[-1]))
        return carry

    if count == per_chunk:
        chunk(0, 0)
    else:
        lax.fori_loop(0, count // per_chunk, chunk, 0)
    for h in range(share):
        if last_part:
            shift_ref[h] = state_ref[h, :, :HEAD_DIM]
            over = jnp.where(is_first == 1, 0.0, state_ref[h, :, HEAD_DIM:])
            map_high, map_low = split(over)
            map_ref[h] = beside(map_high, map_low)
        else:
            final_ref[h] = state_ref[h]

    def drain(n, carry):
        leaving(0, n).wait()
        leaving(1, n).wait()
        leaving_flip(n).wait()
        return carry

    lax.fori_loop(0, count, drain, 0)


def advance_kernel(shift_ref, map_ref, incoming_ref, out_ref):
    for h in range(shift_ref.shape[0]):
        high, low = split(incoming_ref[h])
        row = beside(high, low)
        both = dot(map_ref[h], below(row, row))
        out_ref[h] = shift_ref[h] + both[:, :HEAD_DIM] + both[:, HEAD_DIM:]


def finish_kernel(
    dims,
    meta_ref,
    outer_ref,
    tail_ref,
    weight_ref,
    incoming_ref,
    gain_ref,
    solved_in,
    state_in,
    flip_in,
    *refs,
):
    group, share, counts, query_row, gate_row, tail_place = dims
    count = sum(counts)
    line_refs = refs[: len(counts)]
    out_hbm, out_ref, solved_ref, before_ref, flip_ref, rows_ref, sems = refs[len(counts) :]
    piece_rows = BLOCK // 2
    is_first = meta_ref[meta_ref.shape[0] - 1]
    row_index = lax.broadcasted_iota(jnp.int32, (BLOCK, BLOCK), 0)
    col_index = lax.broadcasted_iota(jnp.int32, (BLOCK, BLOCK), 1)
    inclusive = row_index >= col_index

    def arriving(n):
        at = pl.ds(pl.multiple_of(n * BLOCK, BLOCK), BLOCK)
        return (
            pltpu.make_async_copy(flip_in.at[n], flip_ref.at[n], sems.at[0, n]),
            pltpu.make_async_copy(state_in.at[:, at, :], before_ref.at[:, at, :], sems.at[1, n]),
            pltpu.make_async_copy(solved_in.at[:, at, :], solved_ref.at[:, at, :], sems.at[2, n]),
        )

    def leaving(n):
        return pltpu.make_async_copy(out_ref.at[n], out_hbm.at[n], sems.at[3, n])

    def drain(n, carry):
        leaving(n).wait()
        return carry

    def fetch(n, carry):
        for copy in arriving(n):
            copy.start()
        return carry

    lax.fori_loop(0, count, fetch, 0)
    entry = [split(jnp.where(is_first == 1, 0.0, incoming_ref[h])) for h in range(share)]

    def step(index, carry, first_block, per_step, row_ref):
        spots = [index * per_step + b for b in range(per_step)]
        blocks = [first_block + spot for spot in spots]
        queries, grams = {}, {}
        for b, n in enumerate(blocks):
            lead = jnp.where(is_first == 1, 0.0, tail_ref[tail_place].astype(F32))
            shifted_rows(meta_ref, outer_ref, rows_ref, b, lead, n, query_row)
            active = convolved(rows_ref, b, weight_ref, 0)
            queries[b] = active * (unit_scale(active) * HEAD_DIM ** (-0.5))
        for n in blocks:
            for copy in arriving(n):
                copy.wait()
        for b, n in enumerate(blocks):
            grams[b] = narrow_product(split(queries[b]), split(flip_ref[n]))
        units = [(b, h) for b in range(per_step) for h in range(share)]
        lefts, states, fresh = {}, {}, {}
        for b, h in units:
            n = blocks[b]
            at = group * share + h
            cum, beta = row_ref[0, spots[b]], row_ref[1, spots[b]]
            columns = below(cum, jnp.zeros((BLOCK - 8, BLOCK), F32)).T
            column = jnp.broadcast_to(columns[:, at : at + 1], (BLOCK, BLOCK))
            decay = jnp.exp(jnp.where(inclusive, column - cum[at : at + 1], 0.0))
            attend = jnp.where(inclusive, grams[b] * decay * beta[at : at + 1], 0.0)
            q_high, q_low = split(queries[b] * jnp.exp(column))
            a_high, a_low = split(attend)
            lefts[b, h] = (beside(q_high, a_high), beside(q_low, a_low))
        for b, h in units:
            rows = pl.ds(pl.multiple_of(blocks[b] * BLOCK, BLOCK), BLOCK)
            shift = before_ref[h, rows, :HEAD_DIM]
            over = split(before_ref[h, rows, HEAD_DIM:])
            states[b, h] = split(shift + narrow_product(over, entry[h]))
        for b, h in units:
            rows = pl.ds(pl.multiple_of(blocks[b] * BLOCK, BLOCK), BLOCK)
            px = split(solved_ref[h, rows, HEAD_DIM:])
            ux = solved_ref[h, rows, :HEAD_DIM]
            fresh[b, h] = split(ux - narrow_product(px, states[b, h]))
        for b, h in units:
            n = blocks[b]
            right = below(beside(*states[b, h]), beside(*fresh[b, h]))
            both = dot(lefts[b, h][0], right) + dot(lefts[b, h][1], right)
            core = both[:, :HEAD_DIM] + both[:, HEAD_DIM:]
            scale = lax.rsqrt(jnp.mean(core * core, axis=-1, keepdims=True) + 1e-06)
            gates = []
            for half in range(2):
                place = meta_ref[2 * n + half]
                start = gate_row + h * BLOCK + (place % 2) * piece_rows
                start = pl.multiple_of(start, piece_rows)
                gates.append(outer_ref[place // 2, pl.ds(start, piece_rows), :].astype(F32))
            gate = below(*gates)
            result = core * scale * gain_ref[...] * silu(gate)
            out_ref[n, h * BLOCK : (h + 1) * BLOCK, :] = result.astype(BF16)
            if h == share - 1:
                leaving(n).start()
        return carry

    first_block = 0
    for blocks, row_ref in zip(counts, line_refs):
        per_step = min(4, blocks)
        part = functools.partial(step, first_block=first_block, per_step=per_step, row_ref=row_ref)
        if blocks == per_step:
            part(0, 0)
        else:
            lax.fori_loop(0, blocks // per_step, part, 0)
        first_block += blocks
    lax.fori_loop(0, count, drain, 0)


def gather_kernel(moves, ends, source_count, logit_place, *refs):
    sources, refs = refs[:source_count], list(refs[source_count:])
    logit_ref = refs.pop(0) if logit_place else None
    out_hbm, out_ref, sems, out_sems = refs[:4]
    refs = refs[4:]
    if ends:
        end_sem, end_ref = refs.pop(), refs.pop()
        rows = sources[0].shape[0]
        end_copy = pltpu.make_async_copy(
            sources[0].at[pl.ds(rows - 16, 16), :], end_ref, end_sem.at[0]
        )
        end_copy.start()
    if logit_place:
        wide_ref, plain_ref, logit_sem = refs
        fetch = pltpu.make_async_copy(logit_ref, plain_ref, logit_sem.at[0])
        fetch.start()
    places = out_ref.shape[0]
    copies = [[] for _ in range(places)]
    for number, (source, begin, length, column, place, row) in enumerate(moves):
        copies[place].append(
            pltpu.make_async_copy(
                sources[source].at[pl.ds(begin, length), pl.ds(column, HEAD_DIM)],
                out_ref.at[place, pl.ds(row, length), :],
                sems.at[number],
            )
        )
    for copy in [copy for group in copies for copy in group]:
        copy.start()
    if logit_place:
        first_row, heads = logit_place
        wide_ref[...] = jnp.zeros(wide_ref.shape, F32)
        fetch.wait()
        wide_ref[0 : 2 * VALUE_HEADS, :] = plain_ref[...].astype(F32)
        for place in range(places):
            begin = place * heads
            rates = wide_ref[begin : begin + 8, :]
            steps = wide_ref[VALUE_HEADS + begin : VALUE_HEADS + begin + 8, :]
            out_ref[place, first_row : first_row + 16, :] = below(rates, steps).astype(BF16)
    if ends:
        end_copy.wait()
        for column, place, row in ends:
            out_ref[place, row : row + 16, :] = end_ref[:, column : column + HEAD_DIM]
    leaving = [
        pltpu.make_async_copy(out_ref.at[place], out_hbm.at[place], out_sems.at[place])
        for place in range(places)
    ]
    for place in range(places):
        for copy in copies[place]:
            copy.wait()
        leaving[place].start()
    for copy in leaving:
        copy.wait()


def halo_kernel(places, meta_ref, arrived_ref, out_ref, sems):
    last = meta_ref[meta_ref.shape[0] - 2]
    copies = []
    for tile, row in enumerate(places):
        source = arrived_ref.at[last // 2, pl.ds(row, 16), :]
        copies.append(pltpu.make_async_copy(source, out_ref.at[tile], sems.at[tile]))
    for copy in copies:
        copy.start()
    for copy in copies:
        copy.wait()


def scatter_kernel(moves, *refs):
    source_ref, out_ref, sems = refs[0], refs[-2], refs[-1]
    copies = []
    for number, (place, row, length, column) in enumerate(moves):
        copies.append(
            pltpu.make_async_copy(
                source_ref.at[place, pl.ds(row, length), :],
                out_ref.at[:, pl.ds(column, HEAD_DIM)],
                sems.at[number],
            )
        )
    for copy in copies:
        copy.start()
    for copy in copies:
        copy.wait()


MIB = 2**20
GATHER_MIB = 6
INNER_MIB = 24
FINISH_MIB = 20


def limits(mib):
    return pltpu.CompilerParams(vmem_limit_bytes=mib * MIB)


def cost(flops):
    return pl.CostEstimate(flops=int(flops), bytes_accessed=2**20, transcendentals=0)


vmem = pl.BlockSpec(memory_space=pltpu.VMEM)
smem = pl.BlockSpec(memory_space=pltpu.SMEM)
anywhere = pl.BlockSpec(memory_space=pl.ANY)
stored = pl.BlockSpec(memory_space=pltpu.HBM)


def gather(sources, moves, places, rows, logits=None, first_row=0, heads=0):
    operands, in_specs = list(sources), [anywhere] * len(sources)
    scratch = []
    logit_place = None
    if logits is not None:
        operands.append(logits)
        in_specs.append(anywhere)
        scratch.append(pltpu.VMEM((2 * VALUE_HEADS + 8, logits.shape[1]), F32))
        scratch.append(pltpu.VMEM(logits.shape, BF16))
        scratch.append(pltpu.SemaphoreType.DMA((1,)))
        logit_place = (first_row, heads)
    ends = [(move[3], move[4], move[5]) for move in moves if move[2] == 16]
    moves = [move for move in moves if move[2] != 16]
    scratch = [
        pltpu.VMEM((places, rows, HEAD_DIM), BF16),
        pltpu.SemaphoreType.DMA((len(moves),)),
        pltpu.SemaphoreType.DMA((places,)),
    ] + scratch
    if ends:
        scratch.append(pltpu.VMEM((16, sources[0].shape[1]), BF16))
        scratch.append(pltpu.SemaphoreType.DMA((1,)))
    return pl.pallas_call(
        functools.partial(gather_kernel, tuple(moves), tuple(ends), len(sources), logit_place),
        out_shape=pltpu.HBM((places, rows, HEAD_DIM), BF16),
        in_specs=in_specs,
        out_specs=stored,
        scratch_shapes=scratch,
        compiler_params=limits(GATHER_MIB),
        cost_estimate=cost(8e8),
    )(*operands)


def scatter(source, moves, out_shape, base=None):
    operands, in_specs, aliases = [source], [vmem], {}
    if base is not None:
        operands.append(base)
        in_specs.append(anywhere)
        aliases = {1: 0}
    return pl.pallas_call(
        functools.partial(scatter_kernel, tuple(moves)),
        out_shape=jax.ShapeDtypeStruct(out_shape, BF16),
        in_specs=in_specs,
        out_specs=anywhere,
        scratch_shapes=[pltpu.SemaphoreType.DMA((len(moves),))],
        input_output_aliases=aliases,
        compiler_params=limits(4),
        cost_estimate=cost(8e8),
    )(*operands)


def passed_round(value, axis):
    length = lax.axis_size(axis)
    return lax.ppermute(value, axis, [(i, (i + 1) % length) for i in range(length)])


def exchanged(value):
    return lax.all_to_all(value, "cp", split_axis=0, concat_axis=0, tiled=True)


def per_device(mixed_qkv, gate_z, gate_logits, block_table, conv_weight, a_log, dt_bias, norm_gain):
    cp_count = lax.axis_size("cp")
    seg_count = lax.axis_size("seg")
    cp_place = lax.axis_index("cp")
    rows = mixed_qkv.shape[0]
    heads = VALUE_HEADS // cp_count
    groups = max(1, heads // GROUP)
    share = heads // groups
    tiles = 1 + share
    key_width = KEY_HEADS * HEAD_DIM
    count = cp_count * rows // BLOCK
    gate_row = tiles * BLOCK

    order = jnp.argsort(block_table[0]).astype(jnp.int32)
    is_first = (lax.axis_index("seg") == 0).astype(jnp.int32).reshape(1)
    meta = jnp.concatenate([order, is_first])

    def key_head(place, group):
        return (place * heads + group * share) // GROUP

    def query_column(place, group):
        return key_head(place, group) * HEAD_DIM

    def inner_layout(group):
        later = [other for other in range(1, groups)] if group == 0 else []
        asked = groups if group == 0 else 0
        tail_row = gate_row + 16
        return later, asked, tail_row, tail_row + 16 * (len(later) * tiles + asked)

    def inner_columns(place, group):
        found = [key_width + key_head(place, group) * HEAD_DIM]
        for h in range(share):
            found.append(2 * key_width + (place * heads + group * share + h) * HEAD_DIM)
        return found

    def inner_moves(group):
        later, asked, tail_row, _ = inner_layout(group)
        moves = []
        for place in range(cp_count):
            for tile, column in enumerate(inner_columns(place, group)):
                moves.append((0, 0, rows, column, place, tile * rows))
            extra = [column for other in later for column in inner_columns(place, other)]
            extra += [query_column(place, other) for other in range(asked)]
            for spot, column in enumerate(extra):
                moves.append((0, rows - 16, 16, column, place, tail_row + 16 * spot))
        return moves

    def outer_moves():
        moves = []
        for place in range(cp_count):
            for group in range(groups):
                moves.append((0, 0, rows, query_column(place, group), place, group * rows))
            for h in range(heads):
                column = (place * heads + h) * HEAD_DIM
                moves.append((1, 0, rows, column, place, (groups + h) * rows))
        return moves

    def halo(arrived, places):
        found = pl.pallas_call(
            functools.partial(halo_kernel, tuple(places)),
            out_shape=jax.ShapeDtypeStruct((len(places), 16, HEAD_DIM), BF16),
            in_specs=[smem, anywhere],
            out_specs=vmem,
            scratch_shapes=[pltpu.SemaphoreType.DMA((len(places),))],
            compiler_params=limits(2),
            cost_estimate=cost(1e8),
        )(meta, arrived)
        return passed_round(found, "seg")

    def in_hbm(array):
        return pltpu.with_memory_space_constraint(array, pltpu.HBM)

    received = []
    for group in range(groups):
        later, asked, tail_row, rows_total = inner_layout(group)
        sent = gather(
            [in_hbm(mixed_qkv)],
            inner_moves(group),
            cp_count,
            rows_total,
            logits=in_hbm(gate_logits.T),
            first_row=gate_row,
            heads=heads,
        )
        received.append(exchanged(sent))
        places = [tile * rows + rows - 16 for tile in range(tiles)] if group == 0 else []
        places += [tail_row + 16 * spot for spot in range(len(later) * tiles + asked)]
        if places:
            arrived = halo(received[group], places)
            if group == 0:
                tails = [arrived[other * tiles : (other + 1) * tiles] for other in range(groups)]
            query_tails = arrived[len(places) - asked :]

    packed = gather(
        [in_hbm(mixed_qkv), in_hbm(gate_z)], outer_moves(), cp_count, (groups + heads) * rows
    )
    outer = exchanged(packed)

    shaped = conv_weight.reshape(CONV, -1, HEAD_DIM)

    def taps(first, total):
        return lax.dynamic_slice_in_dim(shaped, first, total, 1).transpose(1, 0, 2)

    weights, query_weights = [], []
    for group in range(groups):
        own_key = key_head(cp_place, group)
        own_value = 2 * KEY_HEADS + cp_place * heads + group * share
        query_weights.append(taps(own_key, 1))
        weights.append(
            jnp.concatenate([taps(KEY_HEADS + own_key, 1), taps(own_value, share)], axis=0)
        )
    head_log = lax.dynamic_slice_in_dim(a_log, cp_place * heads, heads, 0)
    head_bias = lax.dynamic_slice_in_dim(dt_bias, cp_place * heads, heads, 0)
    rates = jnp.pad(jnp.stack([head_log, head_bias]), ((0, 0), (0, 8 - heads)))
    rates = jnp.broadcast_to(rates[:, :, None], (2, 8, BLOCK))

    def inner(group, first_block, blocks, last_part, earlier):
        per_step, per_chunk = min(4, blocks), min(8, blocks)
        dims = (group, share, first_block, blocks, per_step, per_chunk, last_part)
        wide = (share, count * BLOCK, 2 * HEAD_DIM)
        kept = (share, blocks * BLOCK, 2 * HEAD_DIM)
        out_shape = [
            pltpu.HBM(wide, F32),
            pltpu.HBM(wide, F32),
            pltpu.HBM((count, HEAD_DIM, BLOCK), F32),
            jax.ShapeDtypeStruct((2, blocks, 8, BLOCK), F32),
        ]
        if last_part:
            out_shape.append(jax.ShapeDtypeStruct((share, HEAD_DIM, HEAD_DIM), F32))
            out_shape.append(jax.ShapeDtypeStruct((share, HEAD_DIM, 2 * HEAD_DIM), BF16))
        else:
            out_shape.append(jax.ShapeDtypeStruct((share, HEAD_DIM, 2 * HEAD_DIM), F32))
        operands = [meta, received[group], tails[group], weights[group], rates]
        in_specs = [smem] + [vmem] * 4
        aliases = {}
        if earlier is not None:
            state, buffers = earlier
            operands += [state] + list(buffers)
            in_specs += [vmem] + [stored] * 3
            aliases = {6: 0, 7: 1, 8: 2}
        return pl.pallas_call(
            functools.partial(inner_kernel, dims),
            out_shape=out_shape,
            in_specs=in_specs,
            out_specs=[stored] * 3 + [vmem] * (len(out_shape) - 3),
            scratch_shapes=[
                pltpu.VMEM(kept, F32),
                pltpu.VMEM(kept, F32),
                pltpu.VMEM((blocks, HEAD_DIM, BLOCK), F32),
                pltpu.VMEM((per_chunk * tiles, 8 + BLOCK, HEAD_DIM), F32),
                pltpu.VMEM((len(LEVELS), BLOCK, BLOCK), BF16),
                pltpu.VMEM((share, HEAD_DIM, 2 * HEAD_DIM), F32),
                pltpu.SemaphoreType.DMA((3, blocks)),
            ],
            input_output_aliases=aliases,
            compiler_params=limits(INNER_MIB),
            cost_estimate=cost(6e8 * blocks * share),
        )(*operands)

    def chain(shift, over):
        incoming = None
        for rounds in range(seg_count - 1):
            advanced = shift
            if rounds:
                advanced = pl.pallas_call(
                    advance_kernel,
                    out_shape=jax.ShapeDtypeStruct(shift.shape, F32),
                    in_specs=[vmem] * 3,
                    out_specs=vmem,
                    compiler_params=limits(3),
                    cost_estimate=cost(2e8),
                )(shift, over, incoming)
            incoming = passed_round(advanced, "seg")
        if incoming is None:
            incoming = jnp.zeros_like(shift)
        return incoming

    def finish(group, counts, incoming, buffers, lines):
        gate_start = (groups + group * share) * rows
        dims = (group, share, tuple(counts), group * rows, gate_start, group)
        wide = (share, count * BLOCK, 2 * HEAD_DIM)
        operands = [meta, outer, query_tails, query_weights[group], incoming]
        operands.append(norm_gain.reshape(1, HEAD_DIM))
        operands += [in_hbm(array) for array in buffers]
        operands += lines
        return pl.pallas_call(
            functools.partial(finish_kernel, dims),
            out_shape=pltpu.HBM((count, share * BLOCK, HEAD_DIM), BF16),
            in_specs=[smem] + [vmem] * 5 + [stored] * 3 + [vmem] * len(lines),
            out_specs=stored,
            scratch_shapes=[
                pltpu.VMEM((count, share * BLOCK, HEAD_DIM), BF16),
                pltpu.VMEM(wide, F32),
                pltpu.VMEM(wide, F32),
                pltpu.VMEM((count, HEAD_DIM, BLOCK), F32),
                pltpu.VMEM((4, 8 + BLOCK, HEAD_DIM), F32),
                pltpu.SemaphoreType.DMA((4, count)),
            ],
            compiler_params=limits(FINISH_MIB),
            cost_estimate=cost(1.5e9),
        )(*operands)

    result = None
    for group in range(groups):
        parts = 1
        blocks = count // parts
        earlier, lines = None, []
        for part in range(parts):
            *buffers, line, state, over = (
                *inner(group, part * blocks, blocks, part == parts - 1, earlier),
                *([None] if part < parts - 1 else []),
            )
            lines.append(line)
            earlier = (state, buffers)
        incoming = chain(state, over)
        done = finish(group, [blocks] * parts, incoming, buffers, lines)
        swapped = exchanged(done)
        moves = [
            (place, h * rows, rows, (place * heads + group * share + h) * HEAD_DIM)
            for place in range(cp_count)
            for h in range(share)
        ]
        result = scatter(swapped, moves, (rows, VALUE_HEADS * HEAD_DIM), result)
    return result


def solution(mesh):
    return jax.shard_map(
        per_device,
        mesh=mesh,
        in_specs=(
            P(("seg", "cp"), None),
            P(("seg", "cp"), None),
            P(("seg", "cp"), None),
            P("seg", None),
            P(),
            P(),
            P(),
            P(),
        ),
        out_specs=P(("seg", "cp"), None),
        check_vma=False,
    )
```
